128 devices in a mesh: tp: 4 (over x), dp: 32 (over z, y, core).
Axes of the slice: x: 4, y: 4, z: 4, core: 2. Of those that a mesh axis runs over, the one named last changes fastest.
Arguments:
- tokens: int32 [64, 1536], P('dp')
- cotangent: bfloat16 [64, 1536, 1024], P('dp')
- emb_table: bfloat16 [50304, 1024], P('tp')
- w_qkv: bfloat16 [1024, 3072], P(None, 'tp')
- b_qkv: bfloat16 [16, 192], P('tp')
- w_out: bfloat16 [1024, 1024], P('tp')
- b_out: bfloat16 [1024], replicated
- ln1_gain: bfloat16 [1024], replicated
- ln1_bias: bfloat16 [1024], replicated
- w_gate: bfloat16 [1024, 4096], P(None, 'tp')
- b_gate: bfloat16 [4096], P('tp')
- w_lin: bfloat16 [1024, 4096], P(None, 'tp')
- b_lin: bfloat16 [4096], P('tp')
- w_down: bfloat16 [4096, 1024], P('tp')
- b_down: bfloat16 [1024], replicated
- ln2_gain: bfloat16 [1024], replicated
Outputs:
- output 1: float32 [50304, 1024], P('tp')
- output 2: float32 [1024, 3072], P(None, 'tp')
- output 3: float32 [16, 192], P('tp')
- output 4: float32 [1024, 1024], P('tp')
- output 5: float32 [1024], replicated
- output 6: float32 [1024], replicated
- output 7: float32 [1024], replicated
- output 8: float32 [1024, 4096], P(None, 'tp')
- output 9: float32 [4096], P('tp')
- output 10: float32 [1024, 4096], P(None, 'tp')
- output 11: float32 [4096], P('tp')
- output 12: float32 [4096, 1024], P('tp')
- output 13: float32 [1024], replicated
- output 14: float32 [1024], replicated
All inputs are finite; a program needn't handle non-finite values.
Results may differ from the reference program's by a relative error of at most 0.0152027.
Values sent between devices are 32-bit elements.
A program may use at most 1 GiB of HBM per device.

```python
import jax
import jax.numpy as jnp
from jax import lax

VOCAB_SIZE = 50304
D_MODEL = 1024
NUM_HEADS = 16
FFN_DIM = 4096
GLOBAL_BATCH = 64
SEQ_LEN = 1536
HEAD_DIM = D_MODEL // NUM_HEADS
ALPHA = 140.0 ** 0.5
EPS = 1e-5
SHRINK = 0.1
ROPE_BASE = 10000.0


def setup_inputs(seed: int = 0) -> dict:
    root_key = jax.random.key(seed)
    key_list = jax.random.split(root_key, 16)
    id_keys = jax.random.split(key_list[0], 2)
    first_ids = jax.random.randint(id_keys[0], (GLOBAL_BATCH, SEQ_LEN), 0, VOCAB_SIZE, dtype=jnp.int32)
    second_ids = jax.random.randint(id_keys[1], (GLOBAL_BATCH, SEQ_LEN), 0, VOCAB_SIZE, dtype=jnp.int32)
    tokens = jnp.minimum(first_ids, second_ids)
    tokens = tokens.at[0, 0].set(0).at[0, SEQ_LEN - 1].set(VOCAB_SIZE - 1)

    def draw(index, shape, scale, offset):
        return (jax.random.normal(key_list[index], shape, jnp.float32) * scale + offset).astype(jnp.bfloat16)

    return {
        'tokens': tokens,
        'cotangent': draw(1, (GLOBAL_BATCH, SEQ_LEN, D_MODEL), 1.0, 0.0),
        'emb_table': draw(2, (VOCAB_SIZE, D_MODEL), 1.0, 0.0),
        'w_qkv': draw(3, (D_MODEL, 3 * D_MODEL), D_MODEL ** -0.5, 0.0),
        'b_qkv': draw(4, (NUM_HEADS, 3 * HEAD_DIM), 0.3, 0.0),
        'w_out': draw(5, (D_MODEL, D_MODEL), ALPHA * D_MODEL ** -0.5, 0.0),
        'b_out': draw(6, (D_MODEL,), 1.0, 0.0),
        'ln1_gain': draw(7, (D_MODEL,), 0.3, 1.0),
        'ln1_bias': draw(8, (D_MODEL,), 0.3, 0.0),
        'w_gate': draw(9, (D_MODEL, FFN_DIM), D_MODEL ** -0.5, 0.0),
        'b_gate': draw(10, (FFN_DIM,), 0.3, 0.0),
        'w_lin': draw(11, (D_MODEL, FFN_DIM), D_MODEL ** -0.5, 0.0),
        'b_lin': draw(12, (FFN_DIM,), 0.3, 0.0),
        'w_down': draw(13, (FFN_DIM, D_MODEL), ALPHA * FFN_DIM ** -0.5, 0.0),
        'b_down': draw(14, (D_MODEL,), 2.0, 0.0),
        'ln2_gain': draw(15, (D_MODEL,), 0.3, 1.0),
    }


def to_bf16(values):
    return values.astype(jnp.bfloat16).astype(jnp.float32)


def norm_scaled(values, gain):
    mean_val = jnp.mean(values, axis=-1, keepdims=True)
    centered = values - mean_val
    variance = jnp.mean(centered * centered, axis=-1, keepdims=True)
    return centered * lax.rsqrt(variance + EPS) * gain


def rope_tables():
    half_dim = HEAD_DIM // 2
    inv_freq = ROPE_BASE ** (-2.0 * jnp.arange(half_dim, dtype=jnp.float32) / HEAD_DIM)
    angles = jnp.arange(SEQ_LEN, dtype=jnp.float32)[:, None] * inv_freq[None, :]
    return jnp.cos(angles)[:, None, :], jnp.sin(angles)[:, None, :]


def apply_rope(values, cos_tab, sin_tab):
    half_dim = values.shape[-1] // 2
    first_half = values[..., :half_dim]
    second_half = values[..., half_dim:]
    return jnp.concatenate([first_half * cos_tab - second_half * sin_tab, second_half * cos_tab + first_half * sin_tab], axis=-1)


def seq_loss(params, emb_rows, seq_cot):
    (w_qkv, b_qkv, w_out, b_out, ln1_gain, ln1_bias, w_gate, b_gate, w_lin, b_lin, w_down, b_down, ln2_gain) = params
    embedded = SHRINK * emb_rows + (1.0 - SHRINK) * lax.stop_gradient(emb_rows)
    qkv_pre = jnp.dot(embedded, w_qkv, preferred_element_type=jnp.float32) + b_qkv.reshape(-1)
    qkv_all = to_bf16(qkv_pre).reshape(SEQ_LEN, NUM_HEADS, 3, HEAD_DIM)
    cos_tab, sin_tab = rope_tables()
    queries = to_bf16(apply_rope(qkv_all[:, :, 0], cos_tab, sin_tab))
    keys_rot = to_bf16(apply_rope(qkv_all[:, :, 1], cos_tab, sin_tab))
    values = qkv_all[:, :, 2]
    scores = jnp.einsum('qhd,khd->hqk', queries, keys_rot) * HEAD_DIM ** -0.5
    causal = jnp.arange(SEQ_LEN)[:, None] >= jnp.arange(SEQ_LEN)[None, :]
    attn_probs = to_bf16(jax.nn.softmax(jnp.where(causal, scores, -1e30), axis=-1))
    context = to_bf16(jnp.einsum('hqk,khd->qhd', attn_probs, values)).reshape(SEQ_LEN, D_MODEL)
    attn_out = jnp.dot(context, w_out, preferred_element_type=jnp.float32) + b_out
    hidden = to_bf16(norm_scaled(ALPHA * embedded + attn_out, ln1_gain) + ln1_bias)
    gate_pre = jnp.dot(hidden, w_gate, preferred_element_type=jnp.float32) + b_gate
    lin_pre = jnp.dot(hidden, w_lin, preferred_element_type=jnp.float32) + b_lin
    inner_act = to_bf16(jax.nn.gelu(gate_pre, approximate=False) * lin_pre)
    ffn_out = jnp.dot(inner_act, w_down, preferred_element_type=jnp.float32) + b_down
    final_out = norm_scaled(ALPHA * hidden + ffn_out, ln2_gain)
    return jnp.sum(final_out * seq_cot)


def reference(tokens, cotangent, emb_table, w_qkv, b_qkv, w_out, b_out, ln1_gain, ln1_bias, w_gate, b_gate, w_lin, b_lin, w_down, b_down, ln2_gain):
    params = tuple(weight.astype(jnp.float32) for weight in (w_qkv, b_qkv, w_out, b_out, ln1_gain, ln1_bias, w_gate, b_gate, w_lin, b_lin, w_down, b_down, ln2_gain))

    def one_sequence(grad_acc, seq_item):
        seq_tokens, seq_cot = seq_item
        emb_rows = jnp.take(emb_table, seq_tokens, axis=0).astype(jnp.float32)

        def loss_of(prm_all, rows_in):
            return seq_loss(prm_all, rows_in, seq_cot.astype(jnp.float32))

        pull_back = jax.vjp(loss_of, params, emb_rows)[1]
        grad_params, grad_rows = pull_back(jnp.ones((), jnp.float32))
        new_acc = jax.tree.map(lambda acc_val, new_val: acc_val + new_val, grad_acc, grad_params)
        return new_acc, grad_rows

    init_acc = jax.tree.map(lambda prm_item: prm_item * 0.0, params)
    grad_params, grad_rows = lax.scan(one_sequence, init_acc, (tokens, cotangent))
    d_table = jax.ops.segment_sum(grad_rows.reshape(-1, D_MODEL), tokens.reshape(-1), num_segments=VOCAB_SIZE)
    (d_w_qkv, d_b_qkv, d_w_out, d_b_out, d_ln1_gain, d_ln1_bias, d_w_gate, d_b_gate, d_w_lin, d_b_lin, d_w_down, d_b_down, d_ln2_gain) = grad_params
    return (d_table, d_w_qkv, d_b_qkv, d_w_out, d_b_out, d_ln1_gain, d_ln1_bias, d_w_gate, d_b_gate, d_w_lin, d_b_lin, d_w_down, d_b_down, d_ln2_gain)
```

```python
import functools

import jax
import jax.numpy as jnp
from jax import lax
from jax.experimental import pallas as pl
from jax.experimental.pallas import tpu as pltpu
from jax.sharding import Mesh, PartitionSpec as P

ALPHA = 140.0 ** 0.5
EPS = 1e-5
SHRINK = 0.1
ROPE_BASE = 10000.0
F32 = jnp.float32
BF16 = jnp.bfloat16
SWAP = ((0, 1), (1, 0))


def swap(values):
    return lax.ppermute(values, 'c', SWAP)


def unit():
    return 1.0 + (lax.axis_index('x') // lax.axis_size('x')).astype(F32)


def rounded(values):
    return (values * unit()).astype(BF16)


def norm_scaled(values, gain):
    mean_val = jnp.mean(values, axis=-1, keepdims=True)
    centered = values - mean_val
    variance = jnp.mean(centered * centered, axis=-1, keepdims=True)
    return centered * lax.rsqrt(variance + EPS) * gain


def geglu(gate_pre, lin_pre):
    return jax.nn.gelu(gate_pre, approximate=False) * lin_pre


def dot(left, right):
    return jnp.dot(left, right, preferred_element_type=F32)


def dot_tn(left, right):
    return lax.dot_general(left, right, (((0,), (0,)), ((), ())), preferred_element_type=F32)


def dot_nt(left, right):
    return lax.dot_general(left, right, (((1,), (1,)), ((), ())), preferred_element_type=F32)


def rope_tables(seq_len, head_dim):
    half_dim = head_dim // 2
    inv_freq = ROPE_BASE ** (-2.0 * jnp.arange(half_dim, dtype=F32) / head_dim)
    angles = jnp.arange(seq_len, dtype=F32)[:, None] * inv_freq[None, :]
    cos, sin = jnp.cos(angles), jnp.sin(angles)
    return jnp.concatenate([cos, cos, cos, cos], axis=1), jnp.concatenate([-sin, sin, -sin, sin], axis=1)


def lanes_of_head(rows, head):
    lane = lax.broadcasted_iota(jnp.int32, (rows, 128), 1)
    return (lane >= 64) if head else (lane < 64)


def rotate(values):
    lane = lax.broadcasted_iota(jnp.int32, values.shape, 1)
    return jnp.where(lane % 64 < 32, pltpu.roll(values, 96, axis=1), pltpu.roll(values, 32, axis=1))


def only_head(values, head):
    return jnp.where(lanes_of_head(values.shape[0], head), values, jnp.zeros_like(values))


def stage_qkv(core, half, qkv_ref, cos_ref, sin_ref, q_scr, k_scr, v_scr):
    for part in (0, 1):
        local = pl.ds(part * half, half)
        place = pl.ds(pl.multiple_of((core * half + part * half) % (2 * half), half), half)
        cos, sin = cos_ref[place, :], sin_ref[place, :]
        q = qkv_ref[local, 0:128].astype(F32)
        k = qkv_ref[local, 128:256].astype(F32)
        q_scr[place, :] = (q * cos + rotate(q) * sin).astype(BF16) * BF16(0.125)
        k_scr[place, :] = (k * cos + rotate(k) * sin).astype(BF16)
        v_scr[place, :] = qkv_ref[local, 256:384]


def softmax_rows(q_h, k_scr, row0, rows):
    s_diag = dot_nt(q_h, k_scr[row0:row0 + rows, :])
    keep = lax.broadcasted_iota(jnp.int32, (rows, rows), 0) >= lax.broadcasted_iota(jnp.int32, (rows, rows), 1)
    scores = jnp.where(keep, s_diag, -1e30)
    if row0:
        scores = jnp.concatenate([dot_nt(q_h, k_scr[0:row0, :]), scores], axis=1)
    top = jnp.max(scores, axis=1, keepdims=True)
    weights = jnp.exp(scores - top)
    total = jnp.sum(weights, axis=1, keepdims=True)
    return (weights * (1.0 / total)).astype(BF16)


def attn_fwd_kernel(half, rows, core_ref, qkv_ref, cos_ref, sin_ref, ctx_ref, q_scr, k_scr, v_scr, ctx_scr):
    core = core_ref[0]
    seq_len = 2 * half
    stage_qkv(core, half, qkv_ref, cos_ref, sin_ref, q_scr, k_scr, v_scr)
    for row0 in range(0, seq_len, rows):
        q_blk = q_scr[row0:row0 + rows, :]
        v_blk = v_scr[0:row0 + rows, :]
        ctx = jnp.zeros((rows, 128), F32)
        for head in (0, 1):
            probs = softmax_rows(only_head(q_blk, head), k_scr, row0, rows)
            ctx = jnp.where(lanes_of_head(rows, head), dot(probs, v_blk), ctx)
        ctx_scr[row0:row0 + rows, :] = ctx.astype(BF16)
    for part in (0, 1):
        place = pl.ds(pl.multiple_of((core * half + part * half) % seq_len, half), half)
        ctx_ref[part * half:(part + 1) * half, :] = ctx_scr[place, :]


def attn_bwd_kernel(half, rows, core_ref, qkv_ref, dctx_ref, cos_ref, sin_ref, dqkv_ref, dbias_ref,
                    q_scr, k_scr, v_scr, do_scr, dq_scr, dk_scr, dv_scr):
    core = core_ref[0]
    seq_len = 2 * half
    stage_qkv(core, half, qkv_ref, cos_ref, sin_ref, q_scr, k_scr, v_scr)
    for part in (0, 1):
        place = pl.ds(pl.multiple_of((core * half + part * half) % seq_len, half), half)
        do_scr[place, :] = dctx_ref[part * half:(part + 1) * half, :]
    dk_scr[...] = jnp.zeros_like(dk_scr)
    dv_scr[...] = jnp.zeros_like(dv_scr)
    for row0 in range(0, seq_len, rows):
        end = row0 + rows
        q_blk = q_scr[row0:end, :]
        do_blk = do_scr[row0:end, :]
        k_blk = k_scr[0:end, :]
        v_blk = v_scr[0:end, :]
        dq = jnp.zeros((rows, 128), F32)
        for head in (0, 1):
            q_h = only_head(q_blk, head)
            do_h = only_head(do_blk, head)
            probs = softmax_rows(q_h, k_scr, row0, rows)
            d_probs = dot_nt(do_h, v_blk)
            probs_f = probs.astype(F32)
            inner = jnp.sum(d_probs * probs_f, axis=1, keepdims=True)
            d_scores = (probs_f * (d_probs - inner)).astype(BF16)
            dq = jnp.where(lanes_of_head(rows, head), dot(d_scores, k_blk), dq)
            dk_scr[0:end, :] += dot_tn(d_scores, q_h)
            dv_scr[0:end, :] += dot_tn(probs, do_h)
        dq_scr[row0:end, :] = dq * 0.125
    for part in (0, 1):
        place = pl.ds(pl.multiple_of((core * half + part * half) % seq_len, half), half)
        cos, sin = cos_ref[place, :], -sin_ref[place, :]
        dq, dk, dv = dq_scr[place, :], dk_scr[place, :], dv_scr[place, :]
        dq = dq * cos + rotate(dq) * sin
        dk = dk * cos + rotate(dk) * sin
        for place_out, grad in ((0, dq), (128, dk), (256, dv)):
            dqkv_ref[part * half:(part + 1) * half, place_out:place_out + 128] = grad.astype(BF16)
            total = jnp.sum(grad, axis=0, keepdims=True)
            if part:
                dbias_ref[0:1, place_out:place_out + 128] += total
            else:
                dbias_ref[0:1, place_out:place_out + 128] = total


def attention_forward(core, qkv, cos_tab, sin_tab, rows):
    seq_len, width = qkv.shape
    pairs = width // 384
    full = pl.BlockSpec((seq_len, 128), lambda p, c: (0, 0))
    return pl.pallas_call(
        functools.partial(attn_fwd_kernel, seq_len // 2, rows),
        grid_spec=pltpu.PrefetchScalarGridSpec(
            num_scalar_prefetch=1,
            grid=(pairs,),
            in_specs=[pl.BlockSpec((seq_len, 384), lambda p, c: (0, p)), full, full],
            out_specs=pl.BlockSpec((seq_len, 128), lambda p, c: (0, p)),
            scratch_shapes=[pltpu.VMEM((seq_len, 128), BF16)] * 4,
        ),
        out_shape=jax.ShapeDtypeStruct((seq_len, pairs * 128), BF16),
        compiler_params=pltpu.CompilerParams(vmem_limit_bytes=48 * 1024 * 1024),
        cost_estimate=pl.CostEstimate(flops=seq_len * seq_len * 128 * 4 * pairs, bytes_accessed=seq_len * width * 3, transcendentals=seq_len * seq_len * pairs),
        name='attn_fwd',
    )(core, qkv, cos_tab, sin_tab)


def attention_backward(core, qkv, d_ctx, cos_tab, sin_tab, rows):
    seq_len, width = qkv.shape
    pairs = width // 384
    full = pl.BlockSpec((seq_len, 128), lambda p, c: (0, 0))
    return pl.pallas_call(
        functools.partial(attn_bwd_kernel, seq_len // 2, rows),
        grid_spec=pltpu.PrefetchScalarGridSpec(
            num_scalar_prefetch=1,
            grid=(pairs,),
            in_specs=[pl.BlockSpec((seq_len, 384), lambda p, c: (0, p)), pl.BlockSpec((seq_len, 128), lambda p, c: (0, p)), full, full],
            out_specs=[pl.BlockSpec((seq_len, 384), lambda p, c: (0, p)), pl.BlockSpec((1, 384), lambda p, c: (0, p))],
            scratch_shapes=[pltpu.VMEM((seq_len, 128), BF16)] * 4 + [pltpu.VMEM((seq_len, 128), F32)] * 3,
        ),
        out_shape=[jax.ShapeDtypeStruct((seq_len, width), BF16), jax.ShapeDtypeStruct((1, width), F32)],
        compiler_params=pltpu.CompilerParams(vmem_limit_bytes=56 * 1024 * 1024),
        cost_estimate=pl.CostEstimate(flops=seq_len * seq_len * 128 * 10 * pairs, bytes_accessed=seq_len * width * 5, transcendentals=seq_len * seq_len * pairs),
        name='attn_bwd',
    )(core, qkv, d_ctx, cos_tab, sin_tab)


def pair_order(rows, n_pairs):
    split = rows.reshape(n_pairs, 2, 3, 64, *rows.shape[1:])
    return jnp.swapaxes(split, 1, 2).reshape(rows.shape)


def head_order(rows, n_pairs):
    split = rows.reshape(n_pairs, 3, 2, 64, *rows.shape[1:])
    return jnp.swapaxes(split, 1, 2).reshape(rows.shape)


def solution(mesh):
    n_tp = mesh.shape['tp']
    n_dp = mesh.shape['dp']
    n_q = n_dp // 2
    fine = Mesh(mesh.devices.reshape(n_tp, n_q, 2), ('x', 'q', 'c'))
    col, row, rep, vec = P(None, 'x'), P('x', None), P(), P('x')
    weight_specs = (col, row, row, rep, rep, rep, col, vec, col, vec, row, rep, rep)
    in_specs = (P(('q', 'c'), None), P(('q', 'c'), None, None), row) + weight_specs
    out_specs = (row,) + weight_specs

    def device_step(tokens, cotangent, emb_table, w_qkv, b_qkv, w_out, b_out, ln1_gain, ln1_bias, w_gate, b_gate, w_lin, b_lin, w_down, b_down, ln2_gain):
        xi, qi, ci = lax.axis_index('x'), lax.axis_index('q'), lax.axis_index('c')
        seqs, seq_len = tokens.shape
        half = seq_len // 2
        vocab_loc, width = emb_table.shape
        heads_loc = b_qkv.shape[0]
        pairs_loc = heads_loc // 4
        chips = n_tp * n_q

        def half_of(values, which, axis):
            size = values.shape[axis] // 2
            return lax.dynamic_slice_in_dim(values, which * size, size, axis)

        def share(values, axis):
            size = values.shape[axis] // n_q
            return lax.dynamic_slice_in_dim(values, qi * size, size, axis)

        qkv_cols = w_qkv.shape[1] // 2
        ffn_cols = w_gate.shape[1] // 2
        bias_rows = jnp.concatenate([
            pair_order(half_of(b_qkv.astype(F32), ci, 0).reshape(-1), pairs_loc),
            half_of(b_gate.astype(F32), ci, 0), half_of(b_lin.astype(F32), ci, 0)])
        bias_rows = jnp.pad(bias_rows, (0, -bias_rows.shape[0] % (8 * width))).reshape(-1, width)
        parts = [
            share(pair_order(half_of(w_qkv, ci, 1).T, pairs_loc), 0),
            share(half_of(w_out, ci, 0), 0),
            share(half_of(w_gate, ci, 1).T, 0),
            share(half_of(w_lin, ci, 1).T, 0),
            share(half_of(w_down, ci, 0), 0)]
        starts = [bias_rows.shape[0]]
        for part in parts:
            starts.append(starts[-1] + part.shape[0])
        packed = jnp.concatenate([bias_rows] + [part.astype(F32) for part in parts], axis=0)
        packed = lax.all_gather(packed, ('x', 'q'), axis=0, tiled=True).reshape(n_tp, n_q, -1, width)
        wt_qkv, wf_out, wt_gate, wt_lin, wf_down = [
            rounded(packed[:, :, lo:hi].reshape(-1, width)) for lo, hi in zip(starts[:-1], starts[1:])]
        bias_all = packed[:, 0, :starts[0]].reshape(n_tp, -1)
        bf_qkv = bias_all[:, :qkv_cols].reshape(1, -1)
        bf_gate = bias_all[:, qkv_cols:qkv_cols + ffn_cols].reshape(1, -1)
        bf_lin = bias_all[:, qkv_cols + ffn_cols:qkv_cols + 2 * ffn_cols].reshape(1, -1)

        keep_ids = half_of(tokens, ci, 1)
        other_ids = swap(half_of(tokens, 1 - ci, 1))
        line_ids = jnp.where(ci == 0, jnp.concatenate([keep_ids, other_ids], axis=0), jnp.concatenate([other_ids, keep_ids], axis=0))
        line_ids = line_ids - xi * vocab_loc
        in_shard = (line_ids >= 0) & (line_ids < vocab_loc)
        safe_ids = jnp.where(in_shard, line_ids, 0)
        right = [(i, (i + 1) % n_tp) for i in range(n_tp)]
        left = [(i, (i - 1) % n_tp) for i in range(n_tp)]
        quarter = half // 2

        def rows_for(step, top):
            chip = (xi + step) % n_tp
            at = 0 if top else quarter
            ids = lax.dynamic_slice(safe_ids, (chip, at), (1, quarter))[0]
            here = lax.dynamic_slice(in_shard, (chip, at), (1, quarter))[0]
            found = emb_table.at[ids].get(mode='promise_in_bounds')
            return jnp.where(here[:, None], found.astype(F32), 0.0)

        top_sum, low_sum = rows_for(-1, True), rows_for(1, False)
        for step in range(2, n_tp + 1):
            top_sum = lax.ppermute(top_sum, 'x', right) + rows_for(-step, True)
            low_sum = lax.ppermute(low_sum, 'x', left) + rows_for(step, False)
        e_own = jnp.concatenate([top_sum, low_sum], axis=0)

        g_seq = lax.dynamic_slice_in_dim(cotangent, xi % seqs, 1, 0)[0]
        g_other = swap(half_of(g_seq, 1 - ci, 0).astype(F32))
        g_own = jnp.where(xi // seqs == ci, half_of(g_seq, ci, 0).astype(F32), g_other)

        core = ci.astype(jnp.int32).reshape(1)
        cos_tab, sin_tab = rope_tables(seq_len, 64)
        blk = min(256, half)

        def both_halves(own):
            wide = own.astype(F32)
            return jnp.concatenate([own, rounded(swap(wide))], axis=0)

        def sum_halves(left, right_of):
            other = swap(right_of(left[half:]))
            return right_of(left[:half]) + other

        emb = both_halves(e_own.astype(BF16))
        qkv = (dot_nt(emb, wt_qkv) + bf_qkv).astype(BF16)
        context = attention_forward(core, qkv, cos_tab, sin_tab, blk)
        attn_out = sum_halves(context, lambda rows: dot(rows, wf_out)) + b_out.astype(F32)
        normed_one, norm_one_pull = jax.vjp(norm_scaled, ALPHA * e_own + attn_out, ln1_gain.astype(F32))
        z_own = (normed_one + ln1_bias.astype(F32)).astype(BF16)
        hidden = both_halves(z_own)
        gate_pre = dot_nt(hidden, wt_gate) + bf_gate
        lin_pre = dot_nt(hidden, wt_lin) + bf_lin
        inner_val, act_pull = jax.vjp(geglu, gate_pre, lin_pre)
        inner_act = inner_val.astype(BF16)
        ffn_out = sum_halves(inner_act, lambda rows: dot(rows, wf_down)) + b_down.astype(F32)
        norm_two_pull = jax.vjp(norm_scaled, ALPHA * z_own.astype(F32) + ffn_out, ln2_gain.astype(F32))[1]

        d_resid_two, d_ln2_gain = norm_two_pull(g_own)
        d_b_down = jnp.sum(d_resid_two, axis=0)
        d_ffn = both_halves(d_resid_two.astype(BF16))
        d_w_down = dot_tn(inner_act, d_ffn)
        d_inner = dot_nt(d_ffn, wf_down).astype(BF16)
        d_gate_pre, d_lin_pre = act_pull(d_inner.astype(F32))
        d_b_gate = jnp.sum(d_gate_pre, axis=0)
        d_b_lin = jnp.sum(d_lin_pre, axis=0)
        d_gate, d_lin = d_gate_pre.astype(BF16), d_lin_pre.astype(BF16)
        d_w_gate = dot_tn(d_gate, hidden)
        d_w_lin = dot_tn(d_lin, hidden)
        other = swap(dot(d_gate[half:], wt_gate) + dot(d_lin[half:], wt_lin))
        d_hidden = ALPHA * d_resid_two + (dot(d_gate[:half], wt_gate) + dot(d_lin[:half], wt_lin) + other)
        d_ln1_bias = jnp.sum(d_hidden, axis=0)
        d_resid_one, d_ln1_gain = norm_one_pull(d_hidden)
        d_b_out = jnp.sum(d_resid_one, axis=0)
        d_attn = both_halves(d_resid_one.astype(BF16))
        d_w_out = dot_tn(context, d_attn)
        d_context = dot_nt(d_attn, wf_out).astype(BF16)
        d_qkv, d_b_qkv = attention_backward(core, qkv, d_context, cos_tab, sin_tab, blk)
        d_w_qkv = dot_tn(d_qkv, emb)
        d_emb = ALPHA * d_resid_one + sum_halves(d_qkv, lambda rows: dot(rows, wt_qkv))

        def small_split(values):
            return jnp.pad(values, ((0, 0), (0, -values.shape[1] % (n_q * 8 * width)))).reshape(n_tp, -1, width)

        vec5 = jnp.concatenate([d_b_out, d_ln1_gain, d_ln1_bias, d_b_down, d_ln2_gain])
        small = jnp.concatenate([
            jnp.broadcast_to(vec5, (n_tp, vec5.shape[0])),
            d_b_gate.reshape(n_tp, -1), d_b_lin.reshape(n_tp, -1), d_b_qkv.reshape(n_tp, -1)], axis=1)

        def scatter_rows(values):
            return lax.psum_scatter(values, 'q', scatter_dimension=1, tiled=True)

        def to_shard(piece):
            total = lax.dynamic_index_in_dim(piece, xi, 0, keepdims=False)
            for step in range(1, n_tp):
                shift = [(i, (i + step) % n_tp) for i in range(n_tp)]
                total = total + lax.ppermute(lax.dynamic_index_in_dim(piece, (xi + step) % n_tp, 0, keepdims=False), 'x', shift)
            return total

        def by_shard(values):
            return values.reshape(n_tp, -1, width)

        ffn = [
            scatter_rows(by_shard(d_w_down)),
            scatter_rows(jnp.concatenate([by_shard(d_w_gate), by_shard(d_w_lin)], axis=1))]
        attn = jnp.concatenate([by_shard(d_w_qkv), by_shard(d_w_out), small_split(small)], axis=1)

        d_rows = d_emb
        from_left = lax.ppermute(d_rows, 'x', right)
        from_right = lax.ppermute(d_rows, 'x', left)
        far_top = lax.ppermute(from_left[:quarter], 'x', right)
        far_low = lax.ppermute(from_right[quarter:], 'x', left)
        attn, from_left, from_right = lax.optimization_barrier((attn, from_left, from_right))
        attn = scatter_rows(attn)
        order = (xi + jnp.array([0, n_tp - 1, 1, 2], jnp.int32)) % n_tp
        here = in_shard[order].reshape(-1)
        ids = safe_ids[order].reshape(-1)
        d_line = jnp.concatenate([d_rows, from_left, from_right, far_top, far_low], axis=0)
        d_line = jnp.where(here[:, None], d_line, 0.0)
        d_table = jnp.zeros((vocab_loc, width), F32).at[ids].add(d_line, mode='promise_in_bounds')
        ffn, attn, d_table = lax.optimization_barrier((ffn, attn, d_table))
        d_table = lax.psum(d_table, ('q', 'c'))
        pieces = [to_shard(piece) for piece in ffn + [attn]]
        packed_grads, d_table = lax.optimization_barrier((jnp.concatenate(pieces, axis=0), d_table))
        whole = lax.all_gather(packed_grads, ('q', 'c'), axis=0).reshape(n_q, 2, -1, width)

        def unpack(index):
            lo = sum(p.shape[0] for p in pieces[:index])
            return jnp.swapaxes(whole[:, :, lo:lo + pieces[index].shape[0]], 0, 1).reshape(2, -1, width)

        d_w_down = unpack(0).reshape(-1, width)
        gate_lin = unpack(1)
        d_w_gate = gate_lin[:, :ffn_cols].reshape(-1, width).T
        d_w_lin = gate_lin[:, ffn_cols:].reshape(-1, width).T
        attn = unpack(2)
        out_rows = w_out.shape[0] // 2
        d_w_qkv = jnp.concatenate([head_order(attn[i, :qkv_cols], pairs_loc) for i in (0, 1)], axis=0).T
        d_w_out = attn[:, qkv_cols:qkv_cols + out_rows].reshape(-1, width)
        small = attn[:, qkv_cols + out_rows:].reshape(2, -1)
        d_b_out, d_ln1_gain, d_ln1_bias, d_b_down, d_ln2_gain = [
            small[0, i * width:(i + 1) * width] + small[1, i * width:(i + 1) * width] for i in range(5)]
        at = 5 * width
        d_b_gate = small[:, at:at + ffn_cols].reshape(-1)
        d_b_lin = small[:, at + ffn_cols:at + 2 * ffn_cols].reshape(-1)
        at += 2 * ffn_cols
        d_b_qkv = jnp.concatenate([head_order(small[i, at:at + qkv_cols], pairs_loc) for i in (0, 1)]).reshape(heads_loc, -1)
        d_table = SHRINK * d_table
        return (d_table, d_w_qkv, d_b_qkv, d_w_out, d_b_out, d_ln1_gain, d_ln1_bias, d_w_gate, d_b_gate, d_w_lin, d_b_lin, d_w_down, d_b_down, d_ln2_gain)

    return jax.shard_map(device_step, mesh=fine, in_specs=in_specs, out_specs=out_specs, check_vma=False)
```

```python
import functools

import jax
import jax.numpy as jnp
from jax import lax
from jax.experimental import pallas as pl
from jax.experimental.pallas import tpu as pltpu
from jax.sharding import Mesh, PartitionSpec as P

ALPHA = 140.0 ** 0.5
EPS = 1e-5
SHRINK = 0.1
ROPE_BASE = 10000.0
F32 = jnp.float32
BF16 = jnp.bfloat16
SWAP = ((0, 1), (1, 0))


def swap(values):
    return lax.ppermute(values, 'c', SWAP)


def unit():
    return 1.0 + (lax.axis_index('x') // lax.axis_size('x')).astype(F32)


def rounded(values):
    return (values * unit()).astype(BF16)


def norm_scaled(values, gain):
    mean_val = jnp.mean(values, axis=-1, keepdims=True)
    centered = values - mean_val
    variance = jnp.mean(centered * centered, axis=-1, keepdims=True)
    return centered * lax.rsqrt(variance + EPS) * gain


def dot(left, right):
    return jnp.dot(left, right, preferred_element_type=F32)


def dot_tn(left, right):
    return lax.dot_general(left, right, (((0,), (0,)), ((), ())), preferred_element_type=F32)


def dot_nt(left, right):
    return lax.dot_general(left, right, (((1,), (1,)), ((), ())), preferred_element_type=F32)


def rope_tables(seq_len, head_dim):
    half_dim = head_dim // 2
    inv_freq = ROPE_BASE ** (-2.0 * jnp.arange(half_dim, dtype=F32) / head_dim)
    angles = jnp.arange(seq_len, dtype=F32)[:, None] * inv_freq[None, :]
    cos, sin = jnp.cos(angles), jnp.sin(angles)
    return jnp.concatenate([cos, cos, cos, cos], axis=1), jnp.concatenate([-sin, sin, -sin, sin], axis=1)


def lanes_of_head(rows, head):
    lane = lax.broadcasted_iota(jnp.int32, (rows, 128), 1)
    return (lane >= 64) if head else (lane < 64)


def rotate(values):
    lane = lax.broadcasted_iota(jnp.int32, values.shape, 1)
    return jnp.where(lane % 64 < 32, pltpu.roll(values, 96, axis=1), pltpu.roll(values, 32, axis=1))


def only_head(values, head):
    return jnp.where(lanes_of_head(values.shape[0], head), values, jnp.zeros_like(values))


def stage_qkv(core, half, qkv_ref, cos_ref, sin_ref, q_scr, k_scr, v_scr):
    for part in (0, 1):
        local = pl.ds(part * half, half)
        place = pl.ds(pl.multiple_of((core * half + part * half) % (2 * half), half), half)
        cos, sin = cos_ref[place, :], sin_ref[place, :]
        q = qkv_ref[local, 0:128].astype(F32)
        k = qkv_ref[local, 128:256].astype(F32)
        q_scr[place, :] = (q * cos + rotate(q) * sin).astype(BF16) * BF16(0.125)
        k_scr[place, :] = (k * cos + rotate(k) * sin).astype(BF16)
        v_scr[place, :] = qkv_ref[local, 256:384]


def softmax_rows(q_h, k_scr, row0, rows):
    s_diag = dot_nt(q_h, k_scr[row0:row0 + rows, :])
    keep = lax.broadcasted_iota(jnp.int32, (rows, rows), 0) >= lax.broadcasted_iota(jnp.int32, (rows, rows), 1)
    scores = jnp.where(keep, s_diag, -1e30)
    if row0:
        scores = jnp.concatenate([dot_nt(q_h, k_scr[0:row0, :]), scores], axis=1)
    top = jnp.max(scores, axis=1, keepdims=True)
    weights = jnp.exp(scores - top)
    total = jnp.sum(weights, axis=1, keepdims=True)
    return (weights * (1.0 / total)).astype(BF16)


def attn_fwd_kernel(half, rows, core_ref, qkv_ref, cos_ref, sin_ref, ctx_ref, q_scr, k_scr, v_scr, ctx_scr):
    core = core_ref[0]
    seq_len = 2 * half
    stage_qkv(core, half, qkv_ref, cos_ref, sin_ref, q_scr, k_scr, v_scr)
    for row0 in range(0, seq_len, rows):
        q_blk = q_scr[row0:row0 + rows, :]
        v_blk = v_scr[0:row0 + rows, :]
        ctx = jnp.zeros((rows, 128), F32)
        for head in (0, 1):
            probs = softmax_rows(only_head(q_blk, head), k_scr, row0, rows)
            ctx = jnp.where(lanes_of_head(rows, head), dot(probs, v_blk), ctx)
        ctx_scr[row0:row0 + rows, :] = ctx.astype(BF16)
    for part in (0, 1):
        place = pl.ds(pl.multiple_of((core * half + part * half) % seq_len, half), half)
        ctx_ref[part * half:(part + 1) * half, :] = ctx_scr[place, :]


def attn_bwd_kernel(half, rows, core_ref, qkv_ref, dctx_ref, cos_ref, sin_ref, dqkv_ref, dbias_ref,
                    q_scr, k_scr, v_scr, do_scr, dq_scr, dk_scr, dv_scr):
    core = core_ref[0]
    seq_len = 2 * half
    stage_qkv(core, half, qkv_ref, cos_ref, sin_ref, q_scr, k_scr, v_scr)
    for part in (0, 1):
        place = pl.ds(pl.multiple_of((core * half + part * half) % seq_len, half), half)
        do_scr[place, :] = dctx_ref[part * half:(part + 1) * half, :]
    dk_scr[...] = jnp.zeros_like(dk_scr)
    dv_scr[...] = jnp.zeros_like(dv_scr)
    for row0 in range(0, seq_len, rows):
        end = row0 + rows
        q_blk = q_scr[row0:end, :]
        do_blk = do_scr[row0:end, :]
        k_blk = k_scr[0:end, :]
        v_blk = v_scr[0:end, :]
        dq = jnp.zeros((rows, 128), F32)
        for head in (0, 1):
            q_h = only_head(q_blk, head)
            do_h = only_head(do_blk, head)
            probs = softmax_rows(q_h, k_scr, row0, rows)
            d_probs = dot_nt(do_h, v_blk)
            probs_f = probs.astype(F32)
            inner = jnp.sum(d_probs * probs_f, axis=1, keepdims=True)
            d_scores = (probs_f * (d_probs - inner)).astype(BF16)
            dq = jnp.where(lanes_of_head(rows, head), dot(d_scores, k_blk), dq)
            dk_scr[0:end, :] += dot_tn(d_scores, q_h)
            dv_scr[0:end, :] += dot_tn(probs, do_h)
        dq_scr[row0:end, :] = dq * 0.125
    for part in (0, 1):
        place = pl.ds(pl.multiple_of((core * half + part * half) % seq_len, half), half)
        cos, sin = cos_ref[place, :], -sin_ref[place, :]
        dq, dk, dv = dq_scr[place, :], dk_scr[place, :], dv_scr[place, :]
        dq = dq * cos + rotate(dq) * sin
        dk = dk * cos + rotate(dk) * sin
        for place_out, grad in ((0, dq), (128, dk), (256, dv)):
            dqkv_ref[part * half:(part + 1) * half, place_out:place_out + 128] = grad.astype(BF16)
            total = jnp.sum(grad, axis=0, keepdims=True)
            if part:
                dbias_ref[0:1, place_out:place_out + 128] += total
            else:
                dbias_ref[0:1, place_out:place_out + 128] = total


def attention_forward(core, qkv, cos_tab, sin_tab, rows):
    seq_len, width = qkv.shape
    pairs = width // 384
    full = pl.BlockSpec((seq_len, 128), lambda p, c: (0, 0))
    return pl.pallas_call(
        functools.partial(attn_fwd_kernel, seq_len // 2, rows),
        grid_spec=pltpu.PrefetchScalarGridSpec(
            num_scalar_prefetch=1,
            grid=(pairs,),
            in_specs=[pl.BlockSpec((seq_len, 384), lambda p, c: (0, p)), full, full],
            out_specs=pl.BlockSpec((seq_len, 128), lambda p, c: (0, p)),
            scratch_shapes=[pltpu.VMEM((seq_len, 128), BF16)] * 4,
        ),
        out_shape=jax.ShapeDtypeStruct((seq_len, pairs * 128), BF16),
        compiler_params=pltpu.CompilerParams(vmem_limit_bytes=48 * 1024 * 1024),
        cost_estimate=pl.CostEstimate(flops=seq_len * seq_len * 128 * 4 * pairs, bytes_accessed=seq_len * width * 3, transcendentals=seq_len * seq_len * pairs),
        name='attn_fwd',
    )(core, qkv, cos_tab, sin_tab)


def attention_backward(core, qkv, d_ctx, cos_tab, sin_tab, rows):
    seq_len, width = qkv.shape
    pairs = width // 384
    full = pl.BlockSpec((seq_len, 128), lambda p, c: (0, 0))
    return pl.pallas_call(
        functools.partial(attn_bwd_kernel, seq_len // 2, rows),
        grid_spec=pltpu.PrefetchScalarGridSpec(
            num_scalar_prefetch=1,
            grid=(pairs,),
            in_specs=[pl.BlockSpec((seq_len, 384), lambda p, c: (0, p)), pl.BlockSpec((seq_len, 128), lambda p, c: (0, p)), full, full],
            out_specs=[pl.BlockSpec((seq_len, 384), lambda p, c: (0, p)), pl.BlockSpec((1, 384), lambda p, c: (0, p))],
            scratch_shapes=[pltpu.VMEM((seq_len, 128), BF16)] * 4 + [pltpu.VMEM((seq_len, 128), F32)] * 3,
        ),
        out_shape=[jax.ShapeDtypeStruct((seq_len, width), BF16), jax.ShapeDtypeStruct((1, width), F32)],
        compiler_params=pltpu.CompilerParams(vmem_limit_bytes=56 * 1024 * 1024),
        cost_estimate=pl.CostEstimate(flops=seq_len * seq_len * 128 * 10 * pairs, bytes_accessed=seq_len * width * 5, transcendentals=seq_len * seq_len * pairs),
        name='attn_bwd',
    )(core, qkv, d_ctx, cos_tab, sin_tab)


def geglu_fwd_kernel(chunk, hidden_ref, weight_ref, bias_ref, inner_ref, act_ref, slope_ref):
    rows, cols = inner_ref.shape
    for row0 in range(0, rows, chunk):
        place = slice(row0, row0 + chunk)
        part = hidden_ref[place, :]
        gate = dot_nt(part, weight_ref[0:cols, :]) + bias_ref[:, 0:cols]
        lin = dot_nt(part, weight_ref[cols:2 * cols, :]) + bias_ref[:, cols:2 * cols]
        below = 0.5 + 0.5 * lax.erf(gate * (0.5 ** 0.5))
        act = gate * below
        act_ref[place, :] = act
        slope_ref[place, :] = (below + gate * jnp.exp(gate * gate * -0.5) * ((2.0 * jnp.pi) ** -0.5)) * lin
        inner_ref[place, :] = (act * lin).astype(BF16)


def geglu_forward(hidden, weight, bias, groups):
    seq_len, width = hidden.shape
    cols = weight.shape[0] // groups // 2
    tile = pl.BlockSpec((seq_len, cols), lambda i: (0, i))
    shape = (seq_len, groups * cols)
    return pl.pallas_call(
        functools.partial(geglu_fwd_kernel, min(256, seq_len)),
        grid=(groups,),
        in_specs=[pl.BlockSpec((seq_len, width), lambda i: (0, 0)), pl.BlockSpec((2 * cols, width), lambda i: (i, 0)), pl.BlockSpec((1, 2 * cols), lambda i: (0, i))],
        out_specs=[tile, tile, tile],
        out_shape=[jax.ShapeDtypeStruct(shape, BF16), jax.ShapeDtypeStruct(shape, F32), jax.ShapeDtypeStruct(shape, F32)],
        compiler_params=pltpu.CompilerParams(vmem_limit_bytes=56 * 1024 * 1024),
        cost_estimate=pl.CostEstimate(flops=4 * seq_len * width * shape[1], bytes_accessed=seq_len * shape[1] * 10, transcendentals=2 * seq_len * shape[1]),
        name='geglu_fwd',
    )(hidden, weight, bias)


def geglu_bwd_kernel(chunk, d_ffn_ref, weight_ref, act_ref, slope_ref, grad_ref, sum_ref):
    rows, cols = act_ref.shape
    for row0 in range(0, rows, chunk):
        place = slice(row0, row0 + chunk)
        d_inner = dot_nt(d_ffn_ref[place, :], weight_ref[...]).astype(BF16).astype(F32)
        for at, factor in ((0, slope_ref), (cols, act_ref)):
            grad = d_inner * factor[place, :]
            grad_ref[place, at:at + cols] = grad.astype(BF16)
            total = jnp.sum(grad, axis=0, keepdims=True)
            if row0:
                sum_ref[:, at:at + cols] += total
            else:
                sum_ref[:, at:at + cols] = total


def geglu_backward(d_ffn, weight, act, slope, groups):
    seq_len, width = d_ffn.shape
    cols = weight.shape[0] // groups
    tile = pl.BlockSpec((seq_len, cols), lambda i: (0, i))
    return pl.pallas_call(
        functools.partial(geglu_bwd_kernel, min(256, seq_len)),
        grid=(groups,),
        in_specs=[pl.BlockSpec((seq_len, width), lambda i: (0, 0)), pl.BlockSpec((cols, width), lambda i: (i, 0)), tile, tile],
        out_specs=[pl.BlockSpec((seq_len, 2 * cols), lambda i: (0, i)), pl.BlockSpec((1, 2 * cols), lambda i: (0, i))],
        out_shape=[jax.ShapeDtypeStruct((seq_len, 2 * groups * cols), BF16), jax.ShapeDtypeStruct((1, 2 * groups * cols), F32)],
        compiler_params=pltpu.CompilerParams(vmem_limit_bytes=56 * 1024 * 1024),
        cost_estimate=pl.CostEstimate(flops=2 * seq_len * width * groups * cols, bytes_accessed=seq_len * groups * cols * 12, transcendentals=0),
        name='geglu_bwd',
    )(d_ffn, weight, act, slope)


def table_kernel(chunk, ids_ref, *refs):
    blocks, out_ref, table, buf, in_sem, out_sem = refs[:-5], refs[-5], refs[-4], refs[-3], refs[-2], refs[-1]
    vocab = table.shape[0]
    span = vocab // 4
    pieces = []
    first = 0
    for block in blocks:
        for row0 in range(0, block.shape[0], chunk):
            pieces.append((block, row0, first + row0))
        first += block.shape[0]

    def fetch(index):
        block, row0, _ = pieces[index]
        return pltpu.make_async_copy(block.at[pl.ds(row0, chunk), :], buf.at[index % 2], in_sem.at[index % 2])

    fetch(0).start()

    def clear(step, carry):
        table[pl.ds(pl.multiple_of(step * 8, 8), 8), :] = jnp.zeros((8, table.shape[1]), F32)
        return carry

    lax.fori_loop(0, vocab // 8, clear, 0, unroll=4)
    for index, (_, _, base) in enumerate(pieces):
        fetch(index).wait()
        if index + 1 < len(pieces):
            fetch(index + 1).start()

        def add_row(row, carry):
            target = ids_ref[base + row]

            @pl.when(target >= 0)
            def _():
                table[pl.ds(target, 1), :] += buf[index % 2, pl.ds(row, 1), :]

            return carry

        lax.fori_loop(0, chunk, add_row, 0)
    copies = [pltpu.make_async_copy(table.at[pl.ds(i * span, span), :], out_ref.at[pl.ds(i * span, span), :], out_sem.at[i]) for i in range(4)]
    for copy in copies:
        copy.start()
    for copy in copies:
        copy.wait()


def add_rows(ids, blocks, vocab):
    width = blocks[0].shape[1]
    chunk = min(128, blocks[-1].shape[0])
    return pl.pallas_call(
        functools.partial(table_kernel, chunk),
        grid_spec=pltpu.PrefetchScalarGridSpec(
            num_scalar_prefetch=1,
            grid=(),
            in_specs=[pl.BlockSpec(memory_space=pl.ANY)] * len(blocks),
            out_specs=pl.BlockSpec(memory_space=pl.ANY),
            scratch_shapes=[pltpu.VMEM((vocab, width), F32), pltpu.VMEM((2, chunk, width), F32), pltpu.SemaphoreType.DMA((2,)), pltpu.SemaphoreType.DMA((4,))],
        ),
        out_shape=jax.ShapeDtypeStruct((vocab, width), F32),
        compiler_params=pltpu.CompilerParams(vmem_limit_bytes=58 * 1024 * 1024),
        cost_estimate=pl.CostEstimate(flops=30 * vocab * width, bytes_accessed=4 * vocab * width, transcendentals=0),
        name='table_rows',
    )(ids, *blocks)


def ring_blocks(values, axis, n, split=True):
    if n == 1:
        return [(0, values)]
    right = [(i, (i + 1) % n) for i in range(n)]
    left = [(i, (i - 1) % n) for i in range(n)]
    if n == 2:
        return [(0, values), (1, lax.ppermute(values, axis, right))]
    from_left, from_right = lax.ppermute(values, axis, right), lax.ppermute(values, axis, left)
    mid = values.shape[0] // 2
    if split:
        far = jnp.concatenate([lax.ppermute(from_left[:mid], axis, right), lax.ppermute(from_right[mid:], axis, left)], axis=0)
    else:
        far = lax.ppermute(values, axis, [(i, (i + 2) % n) for i in range(n)])
    return [(0, values), (-1, from_left), (1, from_right), (2, far)]


def in_order(blocks, axis, n):
    if n == 1:
        return blocks[0][1][None]
    whole = jnp.zeros((n,) + blocks[0][1].shape, blocks[0][1].dtype)
    for offset, block in blocks:
        whole = lax.dynamic_update_index_in_dim(whole, block, (lax.axis_index(axis) + offset) % n, 0)
    return whole


def pair_order(rows, n_pairs):
    split = rows.reshape(n_pairs, 2, 3, 64, *rows.shape[1:])
    return jnp.swapaxes(split, 1, 2).reshape(rows.shape)


def head_order(rows, n_pairs):
    split = rows.reshape(n_pairs, 3, 2, 64, *rows.shape[1:])
    return jnp.swapaxes(split, 1, 2).reshape(rows.shape)


def solution(mesh):
    n_tp = mesh.shape['tp']
    n_dp = mesh.shape['dp']
    n_q = n_dp // 2
    n_z = 4 if n_q >= 16 else n_q
    n_y = n_q // n_z
    fine = Mesh(mesh.devices.reshape(n_tp, n_z, n_y, 2), ('x', 'z', 'y', 'c'))
    col, row, rep, vec = P(None, 'x'), P('x', None), P(), P('x')
    weight_specs = (col, row, row, rep, rep, rep, col, vec, col, vec, row, rep, rep)
    in_specs = (P(('z', 'y', 'c'), None), P(('z', 'y', 'c'), None, None), row) + weight_specs
    out_specs = (row,) + weight_specs

    def device_step(tokens, cotangent, emb_table, w_qkv, b_qkv, w_out, b_out, ln1_gain, ln1_bias, w_gate, b_gate, w_lin, b_lin, w_down, b_down, ln2_gain):
        xi, ci = lax.axis_index('x'), lax.axis_index('c')
        qi = lax.axis_index(('z', 'y'))
        seqs, seq_len = tokens.shape
        half = seq_len // 2
        vocab_loc, width = emb_table.shape
        heads_loc = b_qkv.shape[0]
        pairs_loc = heads_loc // 4

        def half_of(values, which, axis):
            size = values.shape[axis] // 2
            return lax.dynamic_slice_in_dim(values, which * size, size, axis)

        def share(values, axis):
            size = values.shape[axis] // n_q
            return lax.dynamic_slice_in_dim(values, qi * size, size, axis)

        qkv_cols = w_qkv.shape[1] // 2
        ffn_cols = w_gate.shape[1] // 2
        bias_rows = jnp.concatenate([
            pair_order(half_of(b_qkv.astype(F32), ci, 0).reshape(-1), pairs_loc),
            half_of(b_gate.astype(F32), ci, 0), half_of(b_lin.astype(F32), ci, 0)])
        bias_rows = jnp.pad(bias_rows, (0, -bias_rows.shape[0] % (8 * width))).reshape(-1, width)
        parts = [
            share(pair_order(half_of(w_qkv, ci, 1).T, pairs_loc), 0),
            share(half_of(w_out, ci, 0), 0),
            share(half_of(w_gate, ci, 1).T, 0),
            share(half_of(w_lin, ci, 1).T, 0)]
        starts = [bias_rows.shape[0]]
        for part in parts:
            starts.append(starts[-1] + part.shape[0])
        packed = jnp.concatenate([bias_rows] + [part.astype(F32) for part in parts], axis=0)
        packed = in_order(ring_blocks(packed, 'x', n_tp, split=False), 'x', n_tp)

        def gather_q(values):
            whole = lax.all_gather(values.reshape(-1, width), ('z', 'y'), axis=0, tiled=True)
            return jnp.swapaxes(whole.reshape(n_q, n_tp, -1, width), 0, 1)

        attn_all, ffn_all = gather_q(packed[:, :starts[2]]), gather_q(packed[:, starts[2]:])
        wt_qkv = rounded(attn_all[:, :, starts[0]:starts[1]].reshape(-1, width))
        wf_out = rounded(attn_all[:, :, starts[1]:starts[2]].reshape(-1, width))
        bias_all = attn_all[:, 0, :starts[0]].reshape(n_tp, -1)
        bf_qkv = bias_all[:, :qkv_cols].reshape(1, -1)
        bf_ffn = bias_all[:, qkv_cols:qkv_cols + 2 * ffn_cols].reshape(1, -1)
        wt_ffn = rounded(jnp.swapaxes(ffn_all.reshape(n_tp, n_q, 2, -1, width), 1, 2).reshape(-1, width))

        keep_ids = half_of(tokens, ci, 1)
        other_ids = swap(half_of(tokens, 1 - ci, 1))
        line_ids = jnp.where(ci == 0, jnp.concatenate([keep_ids, other_ids], axis=0), jnp.concatenate([other_ids, keep_ids], axis=0))
        line_ids = line_ids - xi * vocab_loc
        in_shard = (line_ids >= 0) & (line_ids < vocab_loc)
        safe_ids = jnp.where(in_shard, line_ids, 0)
        right = [(i, (i + 1) % n_tp) for i in range(n_tp)]
        left = [(i, (i - 1) % n_tp) for i in range(n_tp)]
        quarter = half // 2
        steps = jnp.arange(1, n_tp + 1, dtype=jnp.int32)
        ring_ids = jnp.stack([
            jnp.take(safe_ids[:, :quarter], (xi - steps) % n_tp, axis=0),
            jnp.take(safe_ids[:, quarter:], (xi + steps) % n_tp, axis=0)], axis=1)
        ring_here = jnp.stack([
            jnp.take(in_shard[:, :quarter], (xi - steps) % n_tp, axis=0),
            jnp.take(in_shard[:, quarter:], (xi + steps) % n_tp, axis=0)], axis=1)
        first_ids, later_ids = ring_ids[:1].reshape(-1), ring_ids[1:].reshape(-1)
        first = emb_table.at[first_ids].get(mode='promise_in_bounds')
        first, later_ids = lax.optimization_barrier((first, later_ids))
        later = emb_table.at[later_ids].get(mode='promise_in_bounds').reshape(n_tp - 1, 2, quarter, width)
        first = first.reshape(2, quarter, width)

        def masked(found, step, way):
            return jnp.where(ring_here[step, way][:, None], found.astype(F32), 0.0)

        top_sum, low_sum = masked(first[0], 0, 0), masked(first[1], 0, 1)
        for step in range(1, n_tp):
            top_sum = lax.ppermute(top_sum, 'x', right) + masked(later[step - 1, 0], step, 0)
            low_sum = lax.ppermute(low_sum, 'x', left) + masked(later[step - 1, 1], step, 1)
        e_own = jnp.concatenate([top_sum, low_sum], axis=0)

        down_own = half_of(w_down, ci, 0).astype(F32)
        e_own, down_own = lax.optimization_barrier((e_own, down_own))
        down_blocks = ring_blocks(down_own, 'x', n_tp)
        wf_down = rounded(in_order(down_blocks, 'x', n_tp).reshape(-1, width))

        g_seq = lax.dynamic_slice_in_dim(cotangent, xi % seqs, 1, 0)[0]
        g_other = swap(half_of(g_seq, 1 - ci, 0).astype(F32))
        g_own = jnp.where(xi // seqs == ci, half_of(g_seq, ci, 0).astype(F32), g_other)

        core = ci.astype(jnp.int32).reshape(1)
        cos_tab, sin_tab = rope_tables(seq_len, 64)
        blk = min(256, half)

        def both_halves(own):
            wide = own.astype(F32)
            return jnp.concatenate([own, rounded(swap(wide))], axis=0)

        def sum_halves(left, right_of):
            other = swap(right_of(left[half:]))
            return right_of(left[:half]) + other

        emb = both_halves(e_own.astype(BF16))
        qkv = (dot_nt(emb, wt_qkv) + bf_qkv).astype(BF16)
        context = attention_forward(core, qkv, cos_tab, sin_tab, blk)
        attn_out = sum_halves(context, lambda rows: dot(rows, wf_out)) + b_out.astype(F32)
        normed_one, norm_one_pull = jax.vjp(norm_scaled, ALPHA * e_own + attn_out, ln1_gain.astype(F32))
        z_own = (normed_one + ln1_bias.astype(F32)).astype(BF16)
        hidden = both_halves(z_own)
        inner_act, act, slope = geglu_forward(hidden, wt_ffn, bf_ffn, n_tp)
        ffn_out = sum_halves(inner_act, lambda rows: dot(rows, wf_down)) + b_down.astype(F32)
        norm_two_pull = jax.vjp(norm_scaled, ALPHA * z_own.astype(F32) + ffn_out, ln2_gain.astype(F32))[1]

        d_resid_two, d_ln2_gain = norm_two_pull(g_own)
        d_b_down = jnp.sum(d_resid_two, axis=0)
        d_ffn = both_halves(d_resid_two.astype(BF16))
        d_w_down = dot_tn(inner_act, d_ffn)
        d_pre, d_b_ffn = geglu_backward(d_ffn, wf_down, act, slope, n_tp)
        d_w_ffn = dot_tn(d_pre, hidden)
        d_hidden = ALPHA * d_resid_two + sum_halves(d_pre, lambda rows: dot(rows, wt_ffn))
        d_ln1_bias = jnp.sum(d_hidden, axis=0)
        d_resid_one, d_ln1_gain = norm_one_pull(d_hidden)
        d_b_out = jnp.sum(d_resid_one, axis=0)
        d_attn = both_halves(d_resid_one.astype(BF16))
        d_w_out = dot_tn(context, d_attn)
        d_context = dot_nt(d_attn, wf_out).astype(BF16)
        d_qkv, d_b_qkv = attention_backward(core, qkv, d_context, cos_tab, sin_tab, blk)
        d_w_qkv = dot_tn(d_qkv, emb)
        d_emb = ALPHA * d_resid_one + sum_halves(d_qkv, lambda rows: dot(rows, wt_qkv))

        def small_split(values):
            return jnp.pad(values, ((0, 0), (0, -values.shape[1] % (n_q * 8 * width)))).reshape(n_tp, -1, width)

        vec5 = jnp.concatenate([d_b_out, d_ln1_gain, d_ln1_bias, d_b_down, d_ln2_gain])
        small = jnp.concatenate([
            jnp.broadcast_to(vec5, (n_tp, vec5.shape[0])),
            d_b_ffn.reshape(n_tp, -1), d_b_qkv.reshape(n_tp, -1)], axis=1)

        def scatter_rows(values):
            return lax.psum_scatter(values, ('z', 'y'), scatter_dimension=1, tiled=True)

        def to_shard(piece):
            total = lax.dynamic_index_in_dim(piece, xi, 0, keepdims=False)
            for step in range(1, n_tp):
                shift = [(i, (i + step) % n_tp) for i in range(n_tp)]
                total = total + lax.ppermute(lax.dynamic_index_in_dim(piece, (xi + step) % n_tp, 0, keepdims=False), 'x', shift)
            return total

        def by_shard(values):
            return values.reshape(n_tp, -1, width)

        ffn = [
            scatter_rows(by_shard(d_w_down)),
            scatter_rows(by_shard(d_w_ffn))]
        attn = jnp.concatenate([by_shard(d_w_qkv), by_shard(d_w_out), small_split(small)], axis=1)

        d_rows = d_emb
        from_left = lax.ppermute(d_rows, 'x', right)
        from_right = lax.ppermute(d_rows, 'x', left)
        far_top = lax.ppermute(from_left[:quarter], 'x', right)
        far_low = lax.ppermute(from_right[quarter:], 'x', left)
        attn, from_left, from_right = lax.optimization_barrier((attn, from_left, from_right))
        attn = scatter_rows(attn)
        order = (xi + jnp.array([0, n_tp - 1, 1, 2], jnp.int32)) % n_tp
        target_ids = jnp.take(jnp.where(in_shard, line_ids, -1), order, axis=0).reshape(-1)
        d_table = add_rows(target_ids, [d_rows, from_left, from_right, far_top, far_low], vocab_loc)
        ffn, attn, d_table = lax.optimization_barrier((ffn, attn, d_table))
        d_table = SHRINK * lax.psum(d_table, ('z', 'y', 'c'))
        pieces = [to_shard(piece) for piece in ffn + [attn]]
        whole = in_order(ring_blocks(jnp.concatenate(pieces, axis=0), 'y', n_y), 'y', n_y)
        whole = in_order(ring_blocks(whole, 'z', n_z), 'z', n_z).reshape(n_q, -1, width)
        whole = in_order([(0, whole), (1, swap(whole))], 'c', 2)

        def unpack(index):
            lo = sum(p.shape[0] for p in pieces[:index])
            return whole[:, :, lo:lo + pieces[index].shape[0]].reshape(2, -1, width)

        d_w_down = unpack(0).reshape(-1, width)
        gate_lin = unpack(1)
        d_w_gate = gate_lin[:, :ffn_cols].reshape(-1, width).T
        d_w_lin = gate_lin[:, ffn_cols:].reshape(-1, width).T
        attn = unpack(2)
        out_rows = w_out.shape[0] // 2
        d_w_qkv = jnp.concatenate([head_order(attn[i, :qkv_cols], pairs_loc) for i in (0, 1)], axis=0).T
        d_w_out = attn[:, qkv_cols:qkv_cols + out_rows].reshape(-1, width)
        small = attn[:, qkv_cols + out_rows:].reshape(2, -1)
        d_b_out, d_ln1_gain, d_ln1_bias, d_b_down, d_ln2_gain = [
            small[0, i * width:(i + 1) * width] + small[1, i * width:(i + 1) * width] for i in range(5)]
        at = 5 * width
        d_b_gate = small[:, at:at + ffn_cols].reshape(-1)
        d_b_lin = small[:, at + ffn_cols:at + 2 * ffn_cols].reshape(-1)
        at += 2 * ffn_cols
        d_b_qkv = jnp.concatenate([head_order(small[i, at:at + qkv_cols], pairs_loc) for i in (0, 1)]).reshape(heads_loc, -1)
        return (d_table, d_w_qkv, d_b_qkv, d_w_out, d_b_out, d_ln1_gain, d_ln1_bias, d_w_gate, d_b_gate, d_w_lin, d_b_lin, d_w_down, d_b_down, d_ln2_gain)

    return jax.shard_map(device_step, mesh=fine, in_specs=in_specs, out_specs=out_specs, check_vma=False)
```

```python
import functools

import jax
import jax.numpy as jnp
from jax import lax
from jax.experimental import pallas as pl
from jax.experimental.pallas import tpu as pltpu
from jax.sharding import Mesh, PartitionSpec as P


ALPHA = 140.0 ** 0.5
EPS = 1e-5
SHRINK = 0.1
ROPE_BASE = 10000.0
F32 = jnp.float32
BF16 = jnp.bfloat16
SWAP = ((0, 1), (1, 0))


def swap(values):
    return lax.ppermute(values, 'c', SWAP)


def unit():
    return 1.0 + (lax.axis_index('x') // lax.axis_size('x')).astype(F32)


def rounded(values):
    return (values * unit()).astype(BF16)


def norm_scaled(values, gain):
    mean_val = jnp.mean(values, axis=-1, keepdims=True)
    centered = values - mean_val
    variance = jnp.mean(centered * centered, axis=-1, keepdims=True)
    return centered * lax.rsqrt(variance + EPS) * gain


def dot(left, right):
    return jnp.dot(left, right, preferred_element_type=F32)


def dot_tn(left, right):
    return lax.dot_general(left, right, (((0,), (0,)), ((), ())), preferred_element_type=F32)


def dot_nt(left, right):
    return lax.dot_general(left, right, (((1,), (1,)), ((), ())), preferred_element_type=F32)


def rope_tables(seq_len, head_dim):
    half_dim = head_dim // 2
    inv_freq = ROPE_BASE ** (-2.0 * jnp.arange(half_dim, dtype=F32) / head_dim)
    angles = jnp.arange(seq_len, dtype=F32)[:, None] * inv_freq[None, :]
    cos, sin = jnp.cos(angles), jnp.sin(angles)
    return jnp.concatenate([cos, cos, cos, cos], axis=1), jnp.concatenate([-sin, sin, -sin, sin], axis=1)


def lanes_of_head(rows, head):
    lane = lax.broadcasted_iota(jnp.int32, (rows, 128), 1)
    return (lane >= 64) if head else (lane < 64)


def rotate(values):
    lane = lax.broadcasted_iota(jnp.int32, values.shape, 1)
    return jnp.where(lane % 64 < 32, pltpu.roll(values, 96, axis=1), pltpu.roll(values, 32, axis=1))


def only_head(values, head):
    return jnp.where(lanes_of_head(values.shape[0], head), values, jnp.zeros_like(values))


def stage_qkv(core, half, qkv_ref, cos_ref, sin_ref, q_scr, k_scr, v_scr):
    for part in (0, 1):
        local = pl.ds(part * half, half)
        place = pl.ds(pl.multiple_of((core * half + part * half) % (2 * half), half), half)
        cos, sin = cos_ref[place, :], sin_ref[place, :]
        q = qkv_ref[local, 0:128].astype(F32)
        k = qkv_ref[local, 128:256].astype(F32)
        q_scr[place, :] = (q * cos + rotate(q) * sin).astype(BF16) * BF16(0.125)
        k_scr[place, :] = (k * cos + rotate(k) * sin).astype(BF16)
        v_scr[place, :] = qkv_ref[local, 256:384]


def softmax_rows(q_h, k_scr, row0, rows):
    s_diag = dot_nt(q_h, k_scr[row0:row0 + rows, :])
    keep = lax.broadcasted_iota(jnp.int32, (rows, rows), 0) >= lax.broadcasted_iota(jnp.int32, (rows, rows), 1)
    scores = jnp.where(keep, s_diag, -1e30)
    if row0:
        scores = jnp.concatenate([dot_nt(q_h, k_scr[0:row0, :]), scores], axis=1)
    top = jnp.max(scores, axis=1, keepdims=True)
    weights = jnp.exp(scores - top)
    total = jnp.sum(weights, axis=1, keepdims=True)
    return (weights * (1.0 / total)).astype(BF16)


def attn_fwd_kernel(half, rows, core_ref, qkv_ref, cos_ref, sin_ref, ctx_ref, q_scr, k_scr, v_scr, ctx_scr):
    core = core_ref[0]
    seq_len = 2 * half
    stage_qkv(core, half, qkv_ref, cos_ref, sin_ref, q_scr, k_scr, v_scr)
    for row0 in range(0, seq_len, rows):
        q_blk = q_scr[row0:row0 + rows, :]
        v_blk = v_scr[0:row0 + rows, :]
        ctx = jnp.zeros((rows, 128), F32)
        for head in (0, 1):
            probs = softmax_rows(only_head(q_blk, head), k_scr, row0, rows)
            ctx = jnp.where(lanes_of_head(rows, head), dot(probs, v_blk), ctx)
        ctx_scr[row0:row0 + rows, :] = ctx.astype(BF16)
    for part in (0, 1):
        place = pl.ds(pl.multiple_of((core * half + part * half) % seq_len, half), half)
        ctx_ref[part * half:(part + 1) * half, :] = ctx_scr[place, :]


def attn_bwd_kernel(half, rows, core_ref, qkv_ref, dctx_ref, cos_ref, sin_ref, dqkv_ref, dbias_ref,
                    q_scr, k_scr, v_scr, do_scr, dq_scr, dk_scr, dv_scr):
    core = core_ref[0]
    seq_len = 2 * half
    stage_qkv(core, half, qkv_ref, cos_ref, sin_ref, q_scr, k_scr, v_scr)
    for part in (0, 1):
        place = pl.ds(pl.multiple_of((core * half + part * half) % seq_len, half), half)
        do_scr[place, :] = dctx_ref[part * half:(part + 1) * half, :]
    dk_scr[...] = jnp.zeros_like(dk_scr)
    dv_scr[...] = jnp.zeros_like(dv_scr)
    for row0 in range(0, seq_len, rows):
        end = row0 + rows
        q_blk = q_scr[row0:end, :]
        do_blk = do_scr[row0:end, :]
        k_blk = k_scr[0:end, :]
        v_blk = v_scr[0:end, :]
        dq = jnp.zeros((rows, 128), F32)
        for head in (0, 1):
            q_h = only_head(q_blk, head)
            do_h = only_head(do_blk, head)
            probs = softmax_rows(q_h, k_scr, row0, rows)
            d_probs = dot_nt(do_h, v_blk)
            probs_f = probs.astype(F32)
            inner = jnp.sum(d_probs * probs_f, axis=1, keepdims=True)
            d_scores = (probs_f * (d_probs - inner)).astype(BF16)
            dq = jnp.where(lanes_of_head(rows, head), dot(d_scores, k_blk), dq)
            dk_scr[0:end, :] += dot_tn(d_scores, q_h)
            dv_scr[0:end, :] += dot_tn(probs, do_h)
        dq_scr[row0:end, :] = dq * 0.125
    for part in (0, 1):
        place = pl.ds(pl.multiple_of((core * half + part * half) % seq_len, half), half)
        cos, sin = cos_ref[place, :], -sin_ref[place, :]
        dq, dk, dv = dq_scr[place, :], dk_scr[place, :], dv_scr[place, :]
        dq = dq * cos + rotate(dq) * sin
        dk = dk * cos + rotate(dk) * sin
        for place_out, grad in ((0, dq), (128, dk), (256, dv)):
            dqkv_ref[part * half:(part + 1) * half, place_out:place_out + 128] = grad.astype(BF16)
            total = jnp.sum(grad, axis=0, keepdims=True)
            if part:
                dbias_ref[0:1, place_out:place_out + 128] += total
            else:
                dbias_ref[0:1, place_out:place_out + 128] = total


def attention_forward(core, qkv, cos_tab, sin_tab, rows):
    seq_len, width = qkv.shape
    pairs = width // 384
    full = pl.BlockSpec((seq_len, 128), lambda p, c: (0, 0))
    return pl.pallas_call(
        functools.partial(attn_fwd_kernel, seq_len // 2, rows),
        grid_spec=pltpu.PrefetchScalarGridSpec(
            num_scalar_prefetch=1,
            grid=(pairs,),
            in_specs=[pl.BlockSpec((seq_len, 384), lambda p, c: (0, p)), full, full],
            out_specs=pl.BlockSpec((seq_len, 128), lambda p, c: (0, p)),
            scratch_shapes=[pltpu.VMEM((seq_len, 128), BF16)] * 4,
        ),
        out_shape=jax.ShapeDtypeStruct((seq_len, pairs * 128), BF16),
        compiler_params=pltpu.CompilerParams(vmem_limit_bytes=48 * 1024 * 1024),
        cost_estimate=pl.CostEstimate(flops=seq_len * seq_len * 128 * 4 * pairs, bytes_accessed=seq_len * width * 3, transcendentals=seq_len * seq_len * pairs),
        name='attn_fwd',
    )(core, qkv, cos_tab, sin_tab)


def attention_backward(core, qkv, d_ctx, cos_tab, sin_tab, rows):
    seq_len, width = qkv.shape
    pairs = width // 384
    full = pl.BlockSpec((seq_len, 128), lambda p, c: (0, 0))
    return pl.pallas_call(
        functools.partial(attn_bwd_kernel, seq_len // 2, rows),
        grid_spec=pltpu.PrefetchScalarGridSpec(
            num_scalar_prefetch=1,
            grid=(pairs,),
            in_specs=[pl.BlockSpec((seq_len, 384), lambda p, c: (0, p)), pl.BlockSpec((seq_len, 128), lambda p, c: (0, p)), full, full],
            out_specs=[pl.BlockSpec((seq_len, 384), lambda p, c: (0, p)), pl.BlockSpec((1, 384), lambda p, c: (0, p))],
            scratch_shapes=[pltpu.VMEM((seq_len, 128), BF16)] * 4 + [pltpu.VMEM((seq_len, 128), F32)] * 3,
        ),
        out_shape=[jax.ShapeDtypeStruct((seq_len, width), BF16), jax.ShapeDtypeStruct((1, width), F32)],
        compiler_params=pltpu.CompilerParams(vmem_limit_bytes=56 * 1024 * 1024),
        cost_estimate=pl.CostEstimate(flops=seq_len * seq_len * 128 * 10 * pairs, bytes_accessed=seq_len * width * 5, transcendentals=seq_len * seq_len * pairs),
        name='attn_bwd',
    )(core, qkv, d_ctx, cos_tab, sin_tab)


def geglu_fwd_kernel(chunk, hidden_ref, wide_ref, bias_ref, inner_ref, act_ref, slope_ref, weight_ref):
    rows, cols = inner_ref.shape
    weight_ref[...] = wide_ref[...].reshape(weight_ref.shape).astype(BF16)
    for row0 in range(0, rows, chunk):
        place = slice(row0, row0 + chunk)
        part = hidden_ref[place, :]
        gate = dot_nt(part, weight_ref[0:cols, :]) + bias_ref[:, 0:cols]
        lin = dot_nt(part, weight_ref[cols:2 * cols, :]) + bias_ref[:, cols:2 * cols]
        below = 0.5 + 0.5 * lax.erf(gate * (0.5 ** 0.5))
        act = gate * below
        act_ref[place, :] = act
        slope_ref[place, :] = (below + gate * jnp.exp(gate * gate * -0.5) * ((2.0 * jnp.pi) ** -0.5)) * lin
        inner_ref[place, :] = (act * lin).astype(BF16)


def geglu_forward(hidden, weight, bias, groups):
    seq_len, width = hidden.shape
    slices, _, slice_rows, _ = weight.shape
    cols = slices * slice_rows // 2
    tile = pl.BlockSpec((seq_len, cols), lambda i: (0, i))
    shape = (seq_len, groups * cols)
    return pl.pallas_call(
        functools.partial(geglu_fwd_kernel, min(256, seq_len)),
        grid=(groups,),
        in_specs=[pl.BlockSpec((seq_len, width), lambda i: (0, 0)), pl.BlockSpec((slices, 1, slice_rows, width), lambda i: (0, i, 0, 0)), pl.BlockSpec((1, 2 * cols), lambda i: (0, i))],
        out_specs=[tile, tile, tile, pl.BlockSpec((2 * cols, width), lambda i: (i, 0))],
        out_shape=[jax.ShapeDtypeStruct(shape, BF16), jax.ShapeDtypeStruct(shape, F32), jax.ShapeDtypeStruct(shape, F32), jax.ShapeDtypeStruct((2 * shape[1], width), BF16)],
        compiler_params=pltpu.CompilerParams(vmem_limit_bytes=56 * 1024 * 1024),
        cost_estimate=pl.CostEstimate(flops=4 * seq_len * width * shape[1], bytes_accessed=seq_len * shape[1] * 10, transcendentals=2 * seq_len * shape[1]),
        name='geglu_fwd',
    )(hidden, weight, bias)


def geglu_bwd_kernel(chunk, d_ffn_ref, weight_ref, act_ref, slope_ref, grad_ref, sum_ref):
    rows, cols = act_ref.shape
    for row0 in range(0, rows, chunk):
        place = slice(row0, row0 + chunk)
        d_inner = dot_nt(d_ffn_ref[place, :], weight_ref[...]).astype(BF16).astype(F32)
        for at, factor in ((0, slope_ref), (cols, act_ref)):
            grad = d_inner * factor[place, :]
            grad_ref[place, at:at + cols] = grad.astype(BF16)
            total = jnp.sum(grad, axis=0, keepdims=True)
            if row0:
                sum_ref[:, at:at + cols] += total
            else:
                sum_ref[:, at:at + cols] = total


def geglu_backward(d_ffn, weight, act, slope, groups):
    seq_len, width = d_ffn.shape
    cols = weight.shape[0] // groups
    tile = pl.BlockSpec((seq_len, cols), lambda i: (0, i))
    return pl.pallas_call(
        functools.partial(geglu_bwd_kernel, min(256, seq_len)),
        grid=(groups,),
        in_specs=[pl.BlockSpec((seq_len, width), lambda i: (0, 0)), pl.BlockSpec((cols, width), lambda i: (i, 0)), tile, tile],
        out_specs=[pl.BlockSpec((seq_len, 2 * cols), lambda i: (0, i)), pl.BlockSpec((1, 2 * cols), lambda i: (0, i))],
        out_shape=[jax.ShapeDtypeStruct((seq_len, 2 * groups * cols), BF16), jax.ShapeDtypeStruct((1, 2 * groups * cols), F32)],
        compiler_params=pltpu.CompilerParams(vmem_limit_bytes=56 * 1024 * 1024),
        cost_estimate=pl.CostEstimate(flops=2 * seq_len * width * groups * cols, bytes_accessed=seq_len * groups * cols * 12, transcendentals=0),
        name='geglu_bwd',
    )(d_ffn, weight, act, slope)


def bucket_kernel(streams, group_ref, value_ref, list_ref, count_ref):
    size = group_ref.shape[0] // streams
    for slot in range(streams * 5):
        count_ref[slot] = 0

    def place(step, carry):
        spots = []
        for stream in range(streams):
            group = group_ref[stream * size + step]
            spots.append((stream * 5 + group, value_ref[stream * size + step]))
        filled = [count_ref[slot] for slot, _ in spots]
        for (slot, value), at in zip(spots, filled):
            list_ref[slot * size + at] = value
            count_ref[slot] = at + 1
        return carry

    lax.fori_loop(0, size, place, 0)


def bucket_ids(ids, streams, vocab):
    total = ids.shape[0]
    size = total // streams
    span = vocab // 4
    group = jnp.where(ids < 0, 4, ids // span)
    value = jnp.where(ids < 0, 0, (ids % span) * total + jnp.arange(total, dtype=jnp.int32))
    smem = pl.BlockSpec(memory_space=pltpu.SMEM)
    return pl.pallas_call(
        functools.partial(bucket_kernel, streams),
        in_specs=[smem, smem],
        out_specs=[smem, smem],
        out_shape=[jax.ShapeDtypeStruct((streams * 5 * size,), jnp.int32), jax.ShapeDtypeStruct((streams * 5,), jnp.int32)],
        cost_estimate=pl.CostEstimate(flops=40_000_000, bytes_accessed=20 * total, transcendentals=0),
        name='bucket_ids',
    )(group, value)


def table_kernel(total, streams, list_ref, count_ref, *refs):
    blocks, out_ref, rows, bufs, in_sem, out_sem = refs[:-5], refs[-5], refs[-4], refs[-3], refs[-2], refs[-1]
    span, width = bufs.shape[1:]
    loads = []
    first = 0
    for index, block in enumerate(blocks):
        loads.append(pltpu.make_async_copy(block, rows.at[pl.ds(first, block.shape[0]), :], in_sem.at[index]))
        first += block.shape[0]
    for load in loads:
        load.start()

    def store(group):
        return pltpu.make_async_copy(bufs.at[group % 2], out_ref.at[pl.ds(group * span, span), :], out_sem.at[group % 2])

    for group in range(4):
        buf = bufs.at[group % 2]
        if group >= 2:
            store(group - 2).wait()

        def clear(step, carry):
            buf[pl.ds(pl.multiple_of(step * 8, 8), 8), :] = jnp.zeros((8, width), F32)
            return carry

        lax.fori_loop(0, span // 8, clear, 0, unroll=3 if (span // 8) % 3 == 0 else 1)
        if group == 0:
            for load in loads:
                load.wait()

        for stream in range(streams):
            slot = stream * 5 + group
            base = slot * (total // streams)

            def add_row(index):
                packed = list_ref[base + index]
                target = packed // total
                source = packed - target * total
                buf[pl.ds(target, 1), :] += rows[pl.ds(source, 1), :]

            def add_four(step, carry):
                for k in range(4):
                    add_row(step * 4 + k)
                return carry

            def add_one(index, carry):
                add_row(index)
                return carry

            count = count_ref[slot]
            lax.fori_loop(0, count // 4, add_four, 0)
            lax.fori_loop(count // 4 * 4, count, add_one, 0)
        store(group).start()
    store(2).wait()
    store(3).wait()


def add_rows(lists, counts, blocks, vocab):
    width = blocks[0].shape[1]
    total = sum(block.shape[0] for block in blocks)
    return pl.pallas_call(
        functools.partial(table_kernel, total, counts.shape[0] // 5),
        grid_spec=pltpu.PrefetchScalarGridSpec(
            num_scalar_prefetch=2,
            grid=(),
            in_specs=[pl.BlockSpec(memory_space=pl.ANY)] * len(blocks),
            out_specs=pl.BlockSpec(memory_space=pl.ANY),
            scratch_shapes=[pltpu.VMEM((total, width), F32), pltpu.VMEM((2, vocab // 4, width), F32), pltpu.SemaphoreType.DMA((len(blocks),)), pltpu.SemaphoreType.DMA((2,))],
        ),
        out_shape=jax.ShapeDtypeStruct((vocab, width), F32),
        compiler_params=pltpu.CompilerParams(vmem_limit_bytes=44 * 1024 * 1024),
        cost_estimate=pl.CostEstimate(flops=30 * vocab * width, bytes_accessed=4 * vocab * width, transcendentals=0),
        name='table_rows',
    )(lists, counts, *blocks)


def ring_blocks(values, axis, n, split=True):
    if n == 1:
        return [(0, values)]
    right = [(i, (i + 1) % n) for i in range(n)]
    left = [(i, (i - 1) % n) for i in range(n)]
    if n == 2:
        return [(0, values), (1, lax.ppermute(values, axis, right))]
    from_left, from_right = lax.ppermute(values, axis, right), lax.ppermute(values, axis, left)
    mid = values.shape[0] // 2
    if split:
        far = jnp.concatenate([lax.ppermute(from_left[:mid], axis, right), lax.ppermute(from_right[mid:], axis, left)], axis=0)
    else:
        far = lax.ppermute(values, axis, [(i, (i + 2) % n) for i in range(n)])
    return [(0, values), (-1, from_left), (1, from_right), (2, far)]


def in_order(blocks, axis, n):
    if n == 1:
        return blocks[0][1][None]
    whole = jnp.zeros((n,) + blocks[0][1].shape, blocks[0][1].dtype)
    for offset, block in blocks:
        whole = lax.dynamic_update_index_in_dim(whole, block, (lax.axis_index(axis) + offset) % n, 0)
    return whole


def pair_order(rows, n_pairs):
    split = rows.reshape(n_pairs, 2, 3, 64, *rows.shape[1:])
    return jnp.swapaxes(split, 1, 2).reshape(rows.shape)


def head_order(rows, n_pairs):
    split = rows.reshape(n_pairs, 3, 2, 64, *rows.shape[1:])
    return jnp.swapaxes(split, 1, 2).reshape(rows.shape)


def solution(mesh):
    n_tp = mesh.shape['tp']
    n_dp = mesh.shape['dp']
    n_q = n_dp // 2
    n_z = 4 if n_q >= 16 else n_q
    n_y = n_q // n_z
    fine = Mesh(mesh.devices.reshape(n_tp, n_z, n_y, 2), ('x', 'z', 'y', 'c'))
    col, row, rep, vec = P(None, 'x'), P('x', None), P(), P('x')
    weight_specs = (col, row, row, rep, rep, rep, col, vec, col, vec, row, rep, rep)
    in_specs = (P(('z', 'y', 'c'), None), P(('z', 'y', 'c'), None, None), row) + weight_specs
    out_specs = (row,) + weight_specs

    def device_step(tokens, cotangent, emb_table, w_qkv, b_qkv, w_out, b_out, ln1_gain, ln1_bias, w_gate, b_gate, w_lin, b_lin, w_down, b_down, ln2_gain):
        xi, ci = lax.axis_index('x'), lax.axis_index('c')
        qi = lax.axis_index(('z', 'y'))
        seqs, seq_len = tokens.shape
        half = seq_len // 2
        vocab_loc, width = emb_table.shape
        heads_loc = b_qkv.shape[0]
        pairs_loc = heads_loc // 4

        def half_of(values, which, axis):
            size = values.shape[axis] // 2
            return lax.dynamic_slice_in_dim(values, which * size, size, axis)

        def share(values, axis):
            size = values.shape[axis] // n_q
            return lax.dynamic_slice_in_dim(values, qi * size, size, axis)

        qkv_cols = w_qkv.shape[1] // 2
        ffn_cols = w_gate.shape[1] // 2
        bias_rows = jnp.concatenate([
            pair_order(half_of(b_qkv.astype(F32), ci, 0).reshape(-1), pairs_loc),
            half_of(b_gate.astype(F32), ci, 0), half_of(b_lin.astype(F32), ci, 0)])
        bias_rows = jnp.pad(bias_rows, (0, -bias_rows.shape[0] % (8 * width))).reshape(-1, width)
        gate_lin = jnp.concatenate([half_of(w_gate, ci, 1), half_of(w_lin, ci, 1)], axis=1)
        parts = [
            share(pair_order(half_of(w_qkv, ci, 1).T, pairs_loc), 0),
            share(half_of(w_out, ci, 0), 0),
            share(gate_lin, 1).T]
        starts = [bias_rows.shape[0]]
        for part in parts:
            starts.append(starts[-1] + part.shape[0])
        packed = jnp.concatenate([bias_rows] + [part.astype(F32) for part in parts], axis=0)
        packed_blocks = ring_blocks(packed, 'x', n_tp, split=False)

        other_tokens = swap(tokens)
        line_tokens = jnp.where(ci == 0, jnp.concatenate([tokens, other_tokens], axis=0), jnp.concatenate([other_tokens, tokens], axis=0)) - xi * vocab_loc
        line_ids = half_of(line_tokens, ci, 1)
        in_shard = (line_ids >= 0) & (line_ids < vocab_loc)
        safe_ids = jnp.where(in_shard, line_ids, 0)
        right = [(i, (i + 1) % n_tp) for i in range(n_tp)]
        left = [(i, (i - 1) % n_tp) for i in range(n_tp)]
        quarter = half // 2
        steps = jnp.arange(1, n_tp + 1, dtype=jnp.int32)
        ring_ids = jnp.stack([
            jnp.take(safe_ids[:, :quarter], (xi - steps) % n_tp, axis=0),
            jnp.take(safe_ids[:, quarter:], (xi + steps) % n_tp, axis=0)], axis=1)
        ring_here = jnp.stack([
            jnp.take(in_shard[:, :quarter], (xi - steps) % n_tp, axis=0),
            jnp.take(in_shard[:, quarter:], (xi + steps) % n_tp, axis=0)], axis=1)
        first_ids, later_ids = ring_ids[:1].reshape(-1), ring_ids[1:].reshape(-1)
        first = emb_table.at[first_ids].get(mode='promise_in_bounds')
        offsets = [offset for offset, _ in packed_blocks]
        first, later_ids, packed_values = lax.optimization_barrier((first, later_ids, [block for _, block in packed_blocks]))
        packed = in_order(list(zip(offsets, packed_values)), 'x', n_tp)

        def gather_q(values):
            whole = lax.all_gather(values.reshape(-1, width), ('z', 'y'), axis=0, tiled=True)
            return whole.reshape(n_q, n_tp, -1, width)

        def weight(gathered, lo, hi):
            return rounded(jnp.swapaxes(gathered[:, :, lo:hi], 0, 1).reshape(-1, width))

        attn_all, ffn_all = gather_q(packed[:, :starts[2]]), gather_q(packed[:, starts[2]:])
        wt_qkv = weight(attn_all, starts[0], starts[1])
        wf_out = weight(attn_all, starts[1], starts[2])
        bias_all = attn_all[0, :, :starts[0]].reshape(n_tp, -1)
        bf_qkv = bias_all[:, :qkv_cols].reshape(1, -1)
        bf_ffn = bias_all[:, qkv_cols:qkv_cols + 2 * ffn_cols].reshape(1, -1)

        later = emb_table.at[later_ids].get(mode='promise_in_bounds').reshape(n_tp - 1, 2, quarter, width)
        first = first.reshape(2, quarter, width)

        def masked(found, step, way):
            return jnp.where(ring_here[step, way][:, None], found.astype(F32), 0.0)

        top_sum, low_sum = masked(first[0], 0, 0), masked(first[1], 0, 1)
        cos_tab, sin_tab = rope_tables(seq_len, 64)
        order = (xi + jnp.array([0, n_tp - 1, 1, 2], jnp.int32)) % n_tp
        target_ids = jnp.concatenate([line_ids, half_of(line_tokens, 1 - ci, 1)], axis=1)
        target_ids = jnp.where((target_ids >= 0) & (target_ids < vocab_loc), target_ids, -1)
        target_ids = jnp.take(target_ids, order, axis=0).reshape(-1)
        for step in range(1, n_tp):
            top_in, low_in = lax.ppermute(top_sum, 'x', right), lax.ppermute(low_sum, 'x', left)
            if step == 3:
                top_in, low_in, wt_qkv, wf_out, bf_qkv, bf_ffn, cos_tab, sin_tab = lax.optimization_barrier(
                    (top_in, low_in, wt_qkv, wf_out, bf_qkv, bf_ffn, cos_tab, sin_tab))
            top_sum = top_in + masked(later[step - 1, 0], step, 0)
            low_sum = low_in + masked(later[step - 1, 1], step, 1)
        e_own = jnp.concatenate([top_sum, low_sum], axis=0)

        down_own = half_of(w_down, ci, 0).astype(F32)
        e_own, down_own = lax.optimization_barrier((e_own, down_own))
        down_left, down_right = lax.ppermute(down_own, 'x', right), lax.ppermute(down_own, 'x', left)

        g_seq = lax.dynamic_slice_in_dim(cotangent, xi % seqs, 1, 0)[0]
        g_other = swap(half_of(g_seq, 1 - ci, 0).astype(F32))
        g_own = jnp.where(xi // seqs == ci, half_of(g_seq, ci, 0).astype(F32), g_other)

        core = ci.astype(jnp.int32).reshape(1)
        blk = min(256, half)

        def both_halves(own):
            wide = own.astype(F32)
            return jnp.concatenate([own, rounded(swap(wide))], axis=0)

        def sum_halves(left, right_of):
            other = swap(right_of(left[half:]))
            return lax.optimization_barrier(right_of(left[:half])) + other

        emb = both_halves(e_own.astype(BF16))
        qkv = (dot_nt(emb, wt_qkv) + bf_qkv).astype(BF16)
        context = attention_forward(core, qkv, cos_tab, sin_tab, blk)
        context, down_left, down_right = lax.optimization_barrier((context, down_left, down_right))
        mid = ffn_cols // 2
        down_top, down_low = lax.ppermute(down_left[:mid], 'x', right), lax.ppermute(down_right[mid:], 'x', left)
        near = in_order([(0, rounded(down_own)), (-1, rounded(down_left)), (1, rounded(down_right))], 'x', n_tp)
        attn_out = sum_halves(context, lambda rows: dot(rows, wf_out)) + b_out.astype(F32)
        normed_one, norm_one_pull = jax.vjp(norm_scaled, ALPHA * e_own + attn_out, ln1_gain.astype(F32))
        z_own = (normed_one + ln1_bias.astype(F32)).astype(BF16)
        hidden = both_halves(z_own)
        inner_act, act, slope, wt_ffn = geglu_forward(hidden, ffn_all, bf_ffn, n_tp)
        inner_act, down_top, down_low = lax.optimization_barrier((inner_act, down_top, down_low))
        wf_down = lax.dynamic_update_index_in_dim(near, rounded(jnp.concatenate([down_top, down_low], axis=0)), (xi + 2) % n_tp, 0).reshape(-1, width)
        ffn_out = sum_halves(inner_act, lambda rows: dot(rows, wf_down)) + b_down.astype(F32)
        norm_two_pull = jax.vjp(norm_scaled, ALPHA * z_own.astype(F32) + ffn_out, ln2_gain.astype(F32))[1]

        d_resid_two, d_ln2_gain = norm_two_pull(g_own)
        d_b_down = jnp.sum(d_resid_two, axis=0)
        d_ffn = both_halves(d_resid_two.astype(BF16))

        def scatter_rows(values):
            return lax.psum_scatter(values, ('z', 'y'), scatter_dimension=1, tiled=True)

        def by_shard(values):
            return values.reshape(n_tp, -1, width)

        d_w_down = dot_tn(inner_act, d_ffn)
        down_piece = scatter_rows(by_shard(d_w_down))
        d_pre, d_b_ffn = geglu_backward(d_ffn, wf_down, act, slope, n_tp)
        d_w_ffn = dot_tn(d_pre, hidden)
        ffn_piece = scatter_rows(by_shard(d_w_ffn))
        d_hidden_sum = sum_halves(d_pre, lambda rows: dot(rows, wt_ffn))
        d_hidden = ALPHA * d_resid_two + d_hidden_sum
        d_ln1_bias = jnp.sum(d_hidden, axis=0)
        d_resid_one, d_ln1_gain = norm_one_pull(d_hidden)
        d_b_out = jnp.sum(d_resid_one, axis=0)
        d_attn = both_halves(d_resid_one.astype(BF16))
        d_context = dot_nt(d_attn, wf_out).astype(BF16)
        d_qkv, d_b_qkv = attention_backward(core, qkv, d_context, cos_tab, sin_tab, blk)

        def column_part(which):
            cols = width // 2
            product = dot(d_qkv, lax.dynamic_slice_in_dim(wt_qkv, which * cols, cols, 1))
            direct = ALPHA * lax.dynamic_slice_in_dim(d_resid_one, which * cols, cols, 1)
            return product + jnp.concatenate([direct, jnp.zeros_like(direct)], axis=0)

        sent = column_part(1 - ci)
        other_rows = jnp.concatenate([swap(sent[half:]), swap(sent[:half])], axis=0)
        d_rows = lax.optimization_barrier(column_part(ci)) + other_rows
        from_left, from_right = lax.ppermute(d_rows, 'x', right), lax.ppermute(d_rows, 'x', left)
        d_rows, d_qkv, d_attn = lax.optimization_barrier((d_rows, d_qkv, d_attn))
        d_w_qkv = dot_tn(d_qkv, emb)
        d_w_out = dot_tn(context, d_attn)

        def small_split(values):
            return jnp.pad(values, ((0, 0), (0, -values.shape[1] % (n_q * 8 * width)))).reshape(n_tp, -1, width)

        vec5 = jnp.concatenate([d_b_out, d_ln1_gain, d_ln1_bias, d_b_down, d_ln2_gain])
        small = jnp.concatenate([
            jnp.broadcast_to(vec5, (n_tp, vec5.shape[0])),
            d_b_ffn.reshape(n_tp, -1), d_b_qkv.reshape(n_tp, -1)], axis=1)

        def to_shard(piece):
            total = lax.dynamic_index_in_dim(piece, xi, 0, keepdims=False)
            for step in range(1, n_tp):
                shift = [(i, (i + step) % n_tp) for i in range(n_tp)]
                total = total + lax.ppermute(lax.dynamic_index_in_dim(piece, (xi + step) % n_tp, 0, keepdims=False), 'x', shift)
            return total

        attn = jnp.concatenate([by_shard(d_w_qkv), by_shard(d_w_out), small_split(small)], axis=1)

        attn = scatter_rows(attn)
        far_top = lax.ppermute(from_left[:half], 'x', right)
        far_low = lax.ppermute(from_right[half:], 'x', left)
        row_lists, row_counts = bucket_ids(target_ids, n_tp, vocab_loc)
        d_table = add_rows(row_lists, row_counts, [d_rows, from_left, from_right, far_top, far_low], vocab_loc)
        down_piece, ffn_piece, attn, d_table = lax.optimization_barrier((down_piece, ffn_piece, attn, d_table))
        d_table = lax.psum(d_table, ('z', 'y'))
        down_piece, gate_lin_piece, attn_piece = [to_shard(piece) for piece in (down_piece, ffn_piece, attn)]

        def gather_rows(values, order):
            sizes = {'z': n_z, 'y': n_y}
            for depth, axis in enumerate(order):
                values = in_order(ring_blocks(values, axis, sizes[axis], split=depth == 1), axis, sizes[axis])
            if order == 'zy':
                values = jnp.swapaxes(values, 0, 1)
            values = values.reshape(n_q, -1, width)
            return in_order([(0, values), (1, swap(values))], 'c', 2)

        mixed = gather_rows(jnp.concatenate([down_piece, attn_piece], axis=0), 'yz')
        n_down = down_piece.shape[0]
        d_w_down = mixed[:, :, :n_down].reshape(-1, width)
        gate_lin = gather_rows(gate_lin_piece, 'zy').reshape(2, -1, width)
        d_w_gate = gate_lin[:, :ffn_cols].reshape(-1, width).T
        d_w_lin = gate_lin[:, ffn_cols:].reshape(-1, width).T
        attn = mixed[:, :, n_down:].reshape(2, -1, width)
        out_rows = w_out.shape[0] // 2
        d_w_qkv = jnp.concatenate([head_order(attn[i, :qkv_cols], pairs_loc) for i in (0, 1)], axis=0).T
        d_w_out = attn[:, qkv_cols:qkv_cols + out_rows].reshape(-1, width)
        small = attn[:, qkv_cols + out_rows:].reshape(2, -1)
        d_b_out, d_ln1_gain, d_ln1_bias, d_b_down, d_ln2_gain = [
            small[0, i * width:(i + 1) * width] + small[1, i * width:(i + 1) * width] for i in range(5)]
        at = 5 * width
        d_b_gate = small[:, at:at + ffn_cols].reshape(-1)
        d_b_lin = small[:, at + ffn_cols:at + 2 * ffn_cols].reshape(-1)
        at += 2 * ffn_cols
        d_b_qkv = jnp.concatenate([head_order(small[i, at:at + qkv_cols], pairs_loc) for i in (0, 1)]).reshape(heads_loc, -1)
        d_table, d_w_qkv, d_w_out, d_w_gate, d_w_lin, d_w_down = lax.optimization_barrier((d_table, d_w_qkv, d_w_out, d_w_gate, d_w_lin, d_w_down))
        cols = width // 2
        base = lax.optimization_barrier(jnp.zeros((vocab_loc, width), F32))
        other_table = swap(d_table)
        d_table = lax.dynamic_update_slice_in_dim(base, SHRINK * d_table, ci * cols, 1)
        d_table = lax.dynamic_update_slice_in_dim(d_table, SHRINK * other_table, (1 - ci) * cols, 1)
        return (d_table, d_w_qkv, d_b_qkv, d_w_out, d_b_out, d_ln1_gain, d_ln1_bias, d_w_gate, d_b_gate, d_w_lin, d_b_lin, d_w_down, d_b_down, d_ln2_gain)

    return jax.shard_map(device_step, mesh=fine, in_specs=in_specs, out_specs=out_specs, check_vma=False)
```

```python
import functools

import jax
import jax.numpy as jnp
from jax import lax
from jax.experimental import pallas as pl
from jax.experimental.pallas import tpu as pltpu
from jax.sharding import Mesh, PartitionSpec as P


ALPHA = 140.0 ** 0.5
EPS = 1e-5
SHRINK = 0.1
ROPE_BASE = 10000.0
F32 = jnp.float32
BF16 = jnp.bfloat16
SWAP = ((0, 1), (1, 0))


def swap(values):
    return lax.ppermute(values, 'c', SWAP)


def unit():
    return 1.0 + (lax.axis_index('x') // lax.axis_size('x')).astype(F32)


def rounded(values):
    return (values * unit()).astype(BF16)


def norm_scaled(values, gain):
    mean_val = jnp.mean(values, axis=-1, keepdims=True)
    centered = values - mean_val
    variance = jnp.mean(centered * centered, axis=-1, keepdims=True)
    return centered * lax.rsqrt(variance + EPS) * gain


def dot(left, right):
    return jnp.dot(left, right, preferred_element_type=F32)


def dot_tn(left, right):
    return lax.dot_general(left, right, (((0,), (0,)), ((), ())), preferred_element_type=F32)


def dot_nt(left, right):
    return lax.dot_general(left, right, (((1,), (1,)), ((), ())), preferred_element_type=F32)


def rope_tables(seq_len, head_dim):
    half_dim = head_dim // 2
    inv_freq = ROPE_BASE ** (-2.0 * jnp.arange(half_dim, dtype=F32) / head_dim)
    angles = jnp.arange(seq_len, dtype=F32)[:, None] * inv_freq[None, :]
    cos, sin = jnp.cos(angles), jnp.sin(angles)
    return jnp.concatenate([cos, cos, cos, cos], axis=1), jnp.concatenate([-sin, sin, -sin, sin], axis=1)


def lanes_of_head(rows, head):
    lane = lax.broadcasted_iota(jnp.int32, (rows, 128), 1)
    return (lane >= 64) if head else (lane < 64)


def rotate(values):
    lane = lax.broadcasted_iota(jnp.int32, values.shape, 1)
    return jnp.where(lane % 64 < 32, pltpu.roll(values, 96, axis=1), pltpu.roll(values, 32, axis=1))


def only_head(values, head):
    return jnp.where(lanes_of_head(values.shape[0], head), values, jnp.zeros_like(values))


def stage_qkv(core, half, qkv_ref, cos_ref, sin_ref, q_scr, k_scr, v_scr):
    for part in (0, 1):
        local = pl.ds(part * half, half)
        place = pl.ds(pl.multiple_of((core * half + part * half) % (2 * half), half), half)
        cos, sin = cos_ref[place, :], sin_ref[place, :]
        q = qkv_ref[local, 0:128].astype(F32)
        k = qkv_ref[local, 128:256].astype(F32)
        q_scr[place, :] = (q * cos + rotate(q) * sin).astype(BF16) * BF16(0.125)
        k_scr[place, :] = (k * cos + rotate(k) * sin).astype(BF16)
        v_scr[place, :] = qkv_ref[local, 256:384]


def softmax_rows(q_h, k_scr, row0, rows):
    s_diag = dot_nt(q_h, k_scr[row0:row0 + rows, :])
    keep = lax.broadcasted_iota(jnp.int32, (rows, rows), 0) >= lax.broadcasted_iota(jnp.int32, (rows, rows), 1)
    scores = jnp.where(keep, s_diag, -1e30)
    if row0:
        scores = jnp.concatenate([dot_nt(q_h, k_scr[0:row0, :]), scores], axis=1)
    top = jnp.max(scores, axis=1, keepdims=True)
    weights = jnp.exp(scores - top)
    total = jnp.sum(weights, axis=1, keepdims=True)
    return (weights * (1.0 / total)).astype(BF16)


def attn_fwd_kernel(half, rows, core_ref, qkv_ref, cos_ref, sin_ref, ctx_ref, q_scr, k_scr, v_scr, ctx_scr):
    core = core_ref[0]
    seq_len = 2 * half
    stage_qkv(core, half, qkv_ref, cos_ref, sin_ref, q_scr, k_scr, v_scr)
    for row0 in range(0, seq_len, rows):
        q_blk = q_scr[row0:row0 + rows, :]
        v_blk = v_scr[0:row0 + rows, :]
        ctx = jnp.zeros((rows, 128), F32)
        for head in (0, 1):
            probs = softmax_rows(only_head(q_blk, head), k_scr, row0, rows)
            ctx = jnp.where(lanes_of_head(rows, head), dot(probs, v_blk), ctx)
        ctx_scr[row0:row0 + rows, :] = ctx.astype(BF16)
    for part in (0, 1):
        place = pl.ds(pl.multiple_of((core * half + part * half) % seq_len, half), half)
        ctx_ref[part * half:(part + 1) * half, :] = ctx_scr[place, :]


def attn_bwd_kernel(half, rows, core_ref, qkv_ref, dctx_ref, cos_ref, sin_ref, dqkv_ref, dbias_ref,
                    q_scr, k_scr, v_scr, do_scr, dq_scr, dk_scr, dv_scr):
    core = core_ref[0]
    seq_len = 2 * half
    stage_qkv(core, half, qkv_ref, cos_ref, sin_ref, q_scr, k_scr, v_scr)
    for part in (0, 1):
        place = pl.ds(pl.multiple_of((core * half + part * half) % seq_len, half), half)
        do_scr[place, :] = dctx_ref[part * half:(part + 1) * half, :]
    dk_scr[...] = jnp.zeros_like(dk_scr)
    dv_scr[...] = jnp.zeros_like(dv_scr)
    for row0 in range(0, seq_len, rows):
        end = row0 + rows
        q_blk = q_scr[row0:end, :]
        do_blk = do_scr[row0:end, :]
        k_blk = k_scr[0:end, :]
        v_blk = v_scr[0:end, :]
        dq = jnp.zeros((rows, 128), F32)
        for head in (0, 1):
            q_h = only_head(q_blk, head)
            do_h = only_head(do_blk, head)
            probs = softmax_rows(q_h, k_scr, row0, rows)
            d_probs = dot_nt(do_h, v_blk)
            probs_f = probs.astype(F32)
            inner = jnp.sum(d_probs * probs_f, axis=1, keepdims=True)
            d_scores = (probs_f * (d_probs - inner)).astype(BF16)
            dq = jnp.where(lanes_of_head(rows, head), dot(d_scores, k_blk), dq)
            dk_scr[0:end, :] += dot_tn(d_scores, q_h)
            dv_scr[0:end, :] += dot_tn(probs, do_h)
        dq_scr[row0:end, :] = dq * 0.125
    for part in (0, 1):
        place = pl.ds(pl.multiple_of((core * half + part * half) % seq_len, half), half)
        cos, sin = cos_ref[place, :], -sin_ref[place, :]
        dq, dk, dv = dq_scr[place, :], dk_scr[place, :], dv_scr[place, :]
        dq = dq * cos + rotate(dq) * sin
        dk = dk * cos + rotate(dk) * sin
        for place_out, grad in ((0, dq), (128, dk), (256, dv)):
            dqkv_ref[part * half:(part + 1) * half, place_out:place_out + 128] = grad.astype(BF16)
            total = jnp.sum(grad, axis=0, keepdims=True)
            if part:
                dbias_ref[0:1, place_out:place_out + 128] += total
            else:
                dbias_ref[0:1, place_out:place_out + 128] = total


def attention_forward(core, qkv, cos_tab, sin_tab, rows):
    seq_len, width = qkv.shape
    pairs = width // 384
    full = pl.BlockSpec((seq_len, 128), lambda p, c: (0, 0))
    return pl.pallas_call(
        functools.partial(attn_fwd_kernel, seq_len // 2, rows),
        grid_spec=pltpu.PrefetchScalarGridSpec(
            num_scalar_prefetch=1,
            grid=(pairs,),
            in_specs=[pl.BlockSpec((seq_len, 384), lambda p, c: (0, p)), full, full],
            out_specs=pl.BlockSpec((seq_len, 128), lambda p, c: (0, p)),
            scratch_shapes=[pltpu.VMEM((seq_len, 128), BF16)] * 4,
        ),
        out_shape=jax.ShapeDtypeStruct((seq_len, pairs * 128), BF16),
        compiler_params=pltpu.CompilerParams(vmem_limit_bytes=48 * 1024 * 1024),
        cost_estimate=pl.CostEstimate(flops=seq_len * seq_len * 128 * 4 * pairs, bytes_accessed=seq_len * width * 3, transcendentals=seq_len * seq_len * pairs),
        name='attn_fwd',
    )(core, qkv, cos_tab, sin_tab)


def attention_backward(core, qkv, d_ctx, cos_tab, sin_tab, rows):
    seq_len, width = qkv.shape
    pairs = width // 384
    full = pl.BlockSpec((seq_len, 128), lambda p, c: (0, 0))
    return pl.pallas_call(
        functools.partial(attn_bwd_kernel, seq_len // 2, rows),
        grid_spec=pltpu.PrefetchScalarGridSpec(
            num_scalar_prefetch=1,
            grid=(pairs,),
            in_specs=[pl.BlockSpec((seq_len, 384), lambda p, c: (0, p)), pl.BlockSpec((seq_len, 128), lambda p, c: (0, p)), full, full],
            out_specs=[pl.BlockSpec((seq_len, 384), lambda p, c: (0, p)), pl.BlockSpec((1, 384), lambda p, c: (0, p))],
            scratch_shapes=[pltpu.VMEM((seq_len, 128), BF16)] * 4 + [pltpu.VMEM((seq_len, 128), F32)] * 3,
        ),
        out_shape=[jax.ShapeDtypeStruct((seq_len, width), BF16), jax.ShapeDtypeStruct((1, width), F32)],
        compiler_params=pltpu.CompilerParams(vmem_limit_bytes=56 * 1024 * 1024),
        cost_estimate=pl.CostEstimate(flops=seq_len * seq_len * 128 * 10 * pairs, bytes_accessed=seq_len * width * 5, transcendentals=seq_len * seq_len * pairs),
        name='attn_bwd',
    )(core, qkv, d_ctx, cos_tab, sin_tab)


def geglu_fwd_kernel(chunk, hidden_ref, wide_ref, bias_ref, inner_ref, act_ref, slope_ref, weight_ref):
    rows, cols = inner_ref.shape
    weight_ref[...] = wide_ref[...].reshape(weight_ref.shape).astype(BF16)
    for row0 in range(0, rows, chunk):
        place = slice(row0, row0 + chunk)
        part = hidden_ref[place, :]
        gate = dot_nt(part, weight_ref[0:cols, :]) + bias_ref[:, 0:cols]
        lin = dot_nt(part, weight_ref[cols:2 * cols, :]) + bias_ref[:, cols:2 * cols]
        below = 0.5 + 0.5 * lax.erf(gate * (0.5 ** 0.5))
        act = gate * below
        act_ref[place, :] = act
        slope_ref[place, :] = (below + gate * jnp.exp(gate * gate * -0.5) * ((2.0 * jnp.pi) ** -0.5)) * lin
        inner_ref[place, :] = (act * lin).astype(BF16)


def geglu_forward(hidden, weight, bias, groups):
    seq_len, width = hidden.shape
    slices, _, slice_rows, _ = weight.shape
    cols = slices * slice_rows // 2
    tile = pl.BlockSpec((seq_len, cols), lambda i: (0, i))
    shape = (seq_len, groups * cols)
    return pl.pallas_call(
        functools.partial(geglu_fwd_kernel, min(256, seq_len)),
        grid=(groups,),
        in_specs=[pl.BlockSpec((seq_len, width), lambda i: (0, 0)), pl.BlockSpec((slices, 1, slice_rows, width), lambda i: (0, i, 0, 0)), pl.BlockSpec((1, 2 * cols), lambda i: (0, i))],
        out_specs=[tile, tile, tile, pl.BlockSpec((2 * cols, width), lambda i: (i, 0))],
        out_shape=[jax.ShapeDtypeStruct(shape, BF16), jax.ShapeDtypeStruct(shape, F32), jax.ShapeDtypeStruct(shape, F32), jax.ShapeDtypeStruct((2 * shape[1], width), BF16)],
        compiler_params=pltpu.CompilerParams(vmem_limit_bytes=56 * 1024 * 1024),
        cost_estimate=pl.CostEstimate(flops=4 * seq_len * width * shape[1], bytes_accessed=seq_len * shape[1] * 10, transcendentals=2 * seq_len * shape[1]),
        name='geglu_fwd',
    )(hidden, weight, bias)


def geglu_bwd_kernel(chunk, d_ffn_ref, weight_ref, act_ref, slope_ref, grad_ref, sum_ref):
    rows, cols = act_ref.shape
    for row0 in range(0, rows, chunk):
        place = slice(row0, row0 + chunk)
        d_inner = dot_nt(d_ffn_ref[place, :], weight_ref[...]).astype(BF16).astype(F32)
        for at, factor in ((0, slope_ref), (cols, act_ref)):
            grad = d_inner * factor[place, :]
            grad_ref[place, at:at + cols] = grad.astype(BF16)
            total = jnp.sum(grad, axis=0, keepdims=True)
            if row0:
                sum_ref[:, at:at + cols] += total
            else:
                sum_ref[:, at:at + cols] = total


def geglu_backward(d_ffn, weight, act, slope, groups):
    seq_len, width = d_ffn.shape
    cols = weight.shape[0] // groups
    tile = pl.BlockSpec((seq_len, cols), lambda i: (0, i))
    return pl.pallas_call(
        functools.partial(geglu_bwd_kernel, min(256, seq_len)),
        grid=(groups,),
        in_specs=[pl.BlockSpec((seq_len, width), lambda i: (0, 0)), pl.BlockSpec((cols, width), lambda i: (i, 0)), tile, tile],
        out_specs=[pl.BlockSpec((seq_len, 2 * cols), lambda i: (0, i)), pl.BlockSpec((1, 2 * cols), lambda i: (0, i))],
        out_shape=[jax.ShapeDtypeStruct((seq_len, 2 * groups * cols), BF16), jax.ShapeDtypeStruct((1, 2 * groups * cols), F32)],
        compiler_params=pltpu.CompilerParams(vmem_limit_bytes=56 * 1024 * 1024),
        cost_estimate=pl.CostEstimate(flops=2 * seq_len * width * groups * cols, bytes_accessed=seq_len * groups * cols * 12, transcendentals=0),
        name='geglu_bwd',
    )(d_ffn, weight, act, slope)


def bucket_kernel(streams, group_ref, value_ref, list_ref, count_ref):
    size = group_ref.shape[0] // streams
    for slot in range(streams * 5):
        count_ref[slot] = 0

    def place(step, carry):
        spots = []
        for stream in range(streams):
            group = group_ref[stream * size + step]
            spots.append((stream * 5 + group, value_ref[stream * size + step]))
        filled = [count_ref[slot] for slot, _ in spots]
        for (slot, value), at in zip(spots, filled):
            list_ref[slot * size + at] = value
            count_ref[slot] = at + 1
        return carry

    lax.fori_loop(0, size, place, 0)


def bucket_ids(ids, streams, vocab):
    total = ids.shape[0]
    size = total // streams
    span = vocab // 4
    group = jnp.where(ids < 0, 4, ids // span)
    value = jnp.where(ids < 0, 0, (ids % span) * total + jnp.arange(total, dtype=jnp.int32))
    smem = pl.BlockSpec(memory_space=pltpu.SMEM)
    return pl.pallas_call(
        functools.partial(bucket_kernel, streams),
        in_specs=[smem, smem],
        out_specs=[smem, smem],
        out_shape=[jax.ShapeDtypeStruct((streams * 5 * size,), jnp.int32), jax.ShapeDtypeStruct((streams * 5,), jnp.int32)],
        cost_estimate=pl.CostEstimate(flops=40_000_000, bytes_accessed=20 * total, transcendentals=0),
        name='bucket_ids',
    )(group, value)


def table_kernel(total, streams, list_ref, count_ref, *refs):
    blocks, outs, (rows, even, odd, in_sem, out_sem) = refs[:-9], refs[-9:-5], refs[-5:]
    span, width = odd.shape
    loads = []
    first = 0
    for index, block in enumerate(blocks):
        loads.append(pltpu.make_async_copy(block, rows.at[pl.ds(first, block.shape[0]), :], in_sem.at[index]))
        first += block.shape[0]
    for load in loads:
        load.start()

    def store(group):
        return pltpu.make_async_copy(even.at[group % 2], outs[group], out_sem.at[group % 2])

    for group in range(4):
        buf = even.at[group % 2]
        if group >= 2:
            store(group - 2).wait()

        def clear(step, carry):
            at = pl.ds(pl.multiple_of(step * 8, 8), 8)
            buf[at, :] = jnp.zeros((8, width), F32)
            odd[at, :] = jnp.zeros((8, width), F32)
            return carry

        lax.fori_loop(0, span // 8, clear, 0, unroll=3 if (span // 8) % 3 == 0 else 1)
        if group == 0:
            for load in loads:
                load.wait()

        def add_row(target_buf, stream, index):
            packed = list_ref[(stream * 5 + group) * (total // streams) + index]
            target = packed // total
            source = packed - target * total
            target_buf[pl.ds(target, 1), :] += rows[pl.ds(source, 1), :]

        for left, right in ((0, 1), (2, 3)):
            n_left, n_right = count_ref[left * 5 + group], count_ref[right * 5 + group]
            both = jnp.minimum(n_left, n_right) // 2

            def add_both(step, carry):
                for k in range(2):
                    add_row(buf, left, step * 2 + k)
                    add_row(odd, right, step * 2 + k)
                return carry

            def add_left(index, carry):
                add_row(buf, left, index)
                return carry

            def add_right(index, carry):
                add_row(odd, right, index)
                return carry

            lax.fori_loop(0, both, add_both, 0)
            lax.fori_loop(both * 2, n_left, add_left, 0)
            lax.fori_loop(both * 2, n_right, add_right, 0)

        def merge(step, carry):
            at = pl.ds(pl.multiple_of(step * 8, 8), 8)
            buf[at, :] += odd[at, :]
            return carry

        lax.fori_loop(0, span // 8, merge, 0, unroll=3 if (span // 8) % 3 == 0 else 1)
        store(group).start()
    store(2).wait()
    store(3).wait()


def add_rows(lists, counts, blocks, vocab):
    width = blocks[0].shape[1]
    total = sum(block.shape[0] for block in blocks)
    span = vocab // 4
    return pl.pallas_call(
        functools.partial(table_kernel, total, counts.shape[0] // 5),
        grid_spec=pltpu.PrefetchScalarGridSpec(
            num_scalar_prefetch=2,
            grid=(),
            in_specs=[pl.BlockSpec(memory_space=pl.ANY)] * len(blocks),
            out_specs=[pl.BlockSpec(memory_space=pl.ANY)] * 4,
            scratch_shapes=[pltpu.VMEM((total, width), F32), pltpu.VMEM((2, span, width), F32), pltpu.VMEM((span, width), F32), pltpu.SemaphoreType.DMA((len(blocks),)), pltpu.SemaphoreType.DMA((2,))],
        ),
        out_shape=[jax.ShapeDtypeStruct((span, width), F32)] * 4,
        compiler_params=pltpu.CompilerParams(vmem_limit_bytes=44 * 1024 * 1024),
        cost_estimate=pl.CostEstimate(flops=30 * vocab * width, bytes_accessed=4 * vocab * width, transcendentals=0),
        name='table_rows',
    )(lists, counts, *blocks)


def ring_blocks(values, axis, n, split=True):
    if n == 1:
        return [(0, values)]
    right = [(i, (i + 1) % n) for i in range(n)]
    left = [(i, (i - 1) % n) for i in range(n)]
    if n == 2:
        return [(0, values), (1, lax.ppermute(values, axis, right))]
    from_left, from_right = lax.ppermute(values, axis, right), lax.ppermute(values, axis, left)
    mid = values.shape[0] // 2
    if split:
        far = jnp.concatenate([lax.ppermute(from_left[:mid], axis, right), lax.ppermute(from_right[mid:], axis, left)], axis=0)
    else:
        far = lax.ppermute(values, axis, [(i, (i + 2) % n) for i in range(n)])
    return [(0, values), (-1, from_left), (1, from_right), (2, far)]


def in_order(blocks, axis, n):
    if n == 1:
        return blocks[0][1][None]
    whole = jnp.zeros((n,) + blocks[0][1].shape, blocks[0][1].dtype)
    for offset, block in blocks:
        whole = lax.dynamic_update_index_in_dim(whole, block, (lax.axis_index(axis) + offset) % n, 0)
    return whole


def pair_order(rows, n_pairs):
    split = rows.reshape(n_pairs, 2, 3, 64, *rows.shape[1:])
    return jnp.swapaxes(split, 1, 2).reshape(rows.shape)


def head_order(rows, n_pairs):
    split = rows.reshape(n_pairs, 3, 2, 64, *rows.shape[1:])
    return jnp.swapaxes(split, 1, 2).reshape(rows.shape)


def solution(mesh):
    n_tp = mesh.shape['tp']
    n_dp = mesh.shape['dp']
    n_q = n_dp // 2
    n_z = 4 if n_q >= 16 else n_q
    n_y = n_q // n_z
    fine = Mesh(mesh.devices.reshape(n_tp, n_z, n_y, 2), ('x', 'z', 'y', 'c'))
    col, row, rep, vec = P(None, 'x'), P('x', None), P(), P('x')
    weight_specs = (col, row, row, rep, rep, rep, col, vec, col, vec, row, rep, rep)
    in_specs = (P(('z', 'y', 'c'), None), P(('z', 'y', 'c'), None, None), row) + weight_specs
    out_specs = (row,) + weight_specs

    def device_step(tokens, cotangent, emb_table, w_qkv, b_qkv, w_out, b_out, ln1_gain, ln1_bias, w_gate, b_gate, w_lin, b_lin, w_down, b_down, ln2_gain):
        xi, ci = lax.axis_index('x'), lax.axis_index('c')
        qi = lax.axis_index(('z', 'y'))
        seqs, seq_len = tokens.shape
        half = seq_len // 2
        vocab_loc, width = emb_table.shape
        heads_loc = b_qkv.shape[0]
        pairs_loc = heads_loc // 4

        def half_of(values, which, axis):
            size = values.shape[axis] // 2
            return lax.dynamic_slice_in_dim(values, which * size, size, axis)

        def share(values, axis):
            size = values.shape[axis] // n_q
            return lax.dynamic_slice_in_dim(values, qi * size, size, axis)

        qkv_cols = w_qkv.shape[1] // 2
        ffn_cols = w_gate.shape[1] // 2
        bias_rows = jnp.concatenate([
            pair_order(half_of(b_qkv.astype(F32), ci, 0).reshape(-1), pairs_loc),
            half_of(b_gate.astype(F32), ci, 0), half_of(b_lin.astype(F32), ci, 0)])
        bias_rows = jnp.pad(bias_rows, (0, -bias_rows.shape[0] % (8 * width))).reshape(-1, width)
        gate_lin = jnp.concatenate([half_of(w_gate, ci, 1), half_of(w_lin, ci, 1)], axis=1)
        parts = [
            share(pair_order(half_of(w_qkv, ci, 1).T, pairs_loc), 0),
            share(half_of(w_out, ci, 0), 0),
            share(gate_lin, 1).T]
        starts = [bias_rows.shape[0]]
        for part in parts:
            starts.append(starts[-1] + part.shape[0])
        packed = jnp.concatenate([bias_rows] + [part.astype(F32) for part in parts], axis=0)
        packed_blocks = ring_blocks(packed, 'x', n_tp, split=False)

        other_tokens = swap(tokens)
        line_tokens = jnp.where(ci == 0, jnp.concatenate([tokens, other_tokens], axis=0), jnp.concatenate([other_tokens, tokens], axis=0)) - xi * vocab_loc
        line_ids = half_of(line_tokens, ci, 1)
        in_shard = (line_ids >= 0) & (line_ids < vocab_loc)
        safe_ids = jnp.where(in_shard, line_ids, 0)
        right = [(i, (i + 1) % n_tp) for i in range(n_tp)]
        left = [(i, (i - 1) % n_tp) for i in range(n_tp)]
        quarter = half // 2
        steps = jnp.arange(1, n_tp + 1, dtype=jnp.int32)
        ring_ids = jnp.stack([
            jnp.take(safe_ids[:, :quarter], (xi - steps) % n_tp, axis=0),
            jnp.take(safe_ids[:, quarter:], (xi + steps) % n_tp, axis=0)], axis=1)
        ring_here = jnp.stack([
            jnp.take(in_shard[:, :quarter], (xi - steps) % n_tp, axis=0),
            jnp.take(in_shard[:, quarter:], (xi + steps) % n_tp, axis=0)], axis=1)
        first_ids, later_ids = ring_ids[:1].reshape(-1), ring_ids[1:].reshape(-1)
        first = emb_table.at[first_ids].get(mode='promise_in_bounds')
        offsets = [offset for offset, _ in packed_blocks]
        first, later_ids, packed_values = lax.optimization_barrier((first, later_ids, [block for _, block in packed_blocks]))
        packed = in_order(list(zip(offsets, packed_values)), 'x', n_tp)

        def gather_q(values):
            whole = lax.all_gather(values.reshape(-1, width), ('z', 'y'), axis=0, tiled=True)
            return whole.reshape(n_q, n_tp, -1, width)

        def weight(gathered, lo, hi):
            return rounded(jnp.swapaxes(gathered[:, :, lo:hi], 0, 1).reshape(-1, width))

        attn_all, ffn_all = gather_q(packed[:, :starts[2]]), gather_q(packed[:, starts[2]:])
        wt_qkv = weight(attn_all, starts[0], starts[1])
        wf_out = weight(attn_all, starts[1], starts[2])
        bias_all = attn_all[0, :, :starts[0]].reshape(n_tp, -1)
        bf_qkv = bias_all[:, :qkv_cols].reshape(1, -1)
        bf_ffn = bias_all[:, qkv_cols:qkv_cols + 2 * ffn_cols].reshape(1, -1)

        later = emb_table.at[later_ids].get(mode='promise_in_bounds').reshape(n_tp - 1, 2, quarter, width)
        first = first.reshape(2, quarter, width)

        def masked(found, step, way):
            return jnp.where(ring_here[step, way][:, None], found.astype(F32), 0.0)

        top_sum, low_sum = masked(first[0], 0, 0), masked(first[1], 0, 1)
        cos_tab, sin_tab = rope_tables(seq_len, 64)
        order = (xi + jnp.array([0, n_tp - 1, 1, 2], jnp.int32)) % n_tp
        target_ids = jnp.concatenate([line_ids, half_of(line_tokens, 1 - ci, 1)], axis=1)
        target_ids = jnp.where((target_ids >= 0) & (target_ids < vocab_loc), target_ids, -1)
        target_ids = jnp.take(target_ids, order, axis=0).reshape(-1)
        for step in range(1, n_tp):
            top_in, low_in = lax.ppermute(top_sum, 'x', right), lax.ppermute(low_sum, 'x', left)
            if step == 3:
                top_in, low_in, wt_qkv, wf_out, bf_qkv, bf_ffn, cos_tab, sin_tab = lax.optimization_barrier(
                    (top_in, low_in, wt_qkv, wf_out, bf_qkv, bf_ffn, cos_tab, sin_tab))
            top_sum = top_in + masked(later[step - 1, 0], step, 0)
            low_sum = low_in + masked(later[step - 1, 1], step, 1)
        e_own = jnp.concatenate([top_sum, low_sum], axis=0)

        down_own = half_of(w_down, ci, 0).astype(F32)
        e_own, down_own = lax.optimization_barrier((e_own, down_own))
        down_left, down_right = lax.ppermute(down_own, 'x', right), lax.ppermute(down_own, 'x', left)

        g_seq = lax.dynamic_slice_in_dim(cotangent, xi % seqs, 1, 0)[0]
        g_other = swap(half_of(g_seq, 1 - ci, 0).astype(F32))
        g_own = jnp.where(xi // seqs == ci, half_of(g_seq, ci, 0).astype(F32), g_other)

        core = ci.astype(jnp.int32).reshape(1)
        blk = min(256, half)

        def both_halves(own):
            wide = own.astype(F32)
            return jnp.concatenate([own, rounded(swap(wide))], axis=0)

        def sum_halves(left, right_of):
            other = swap(right_of(left[half:]))
            return lax.optimization_barrier(right_of(left[:half])) + other

        emb = both_halves(e_own.astype(BF16))
        qkv = (dot_nt(emb, wt_qkv) + bf_qkv).astype(BF16)
        context = attention_forward(core, qkv, cos_tab, sin_tab, blk)
        context, down_left, down_right = lax.optimization_barrier((context, down_left, down_right))
        mid = ffn_cols // 2
        down_top, down_low = lax.ppermute(down_left[:mid], 'x', right), lax.ppermute(down_right[mid:], 'x', left)
        near = in_order([(0, rounded(down_own)), (-1, rounded(down_left)), (1, rounded(down_right))], 'x', n_tp)
        attn_out = sum_halves(context, lambda rows: dot(rows, wf_out)) + b_out.astype(F32)
        normed_one, norm_one_pull = jax.vjp(norm_scaled, ALPHA * e_own + attn_out, ln1_gain.astype(F32))
        z_own = (normed_one + ln1_bias.astype(F32)).astype(BF16)
        hidden = both_halves(z_own)
        inner_act, act, slope, wt_ffn = geglu_forward(hidden, ffn_all, bf_ffn, n_tp)
        inner_act, down_top, down_low = lax.optimization_barrier((inner_act, down_top, down_low))
        wf_down = lax.dynamic_update_index_in_dim(near, rounded(jnp.concatenate([down_top, down_low], axis=0)), (xi + 2) % n_tp, 0).reshape(-1, width)
        ffn_out = sum_halves(inner_act, lambda rows: dot(rows, wf_down)) + b_down.astype(F32)
        norm_two_pull = jax.vjp(norm_scaled, ALPHA * z_own.astype(F32) + ffn_out, ln2_gain.astype(F32))[1]

        d_resid_two, d_ln2_gain = norm_two_pull(g_own)
        d_b_down = jnp.sum(d_resid_two, axis=0)
        d_ffn = both_halves(d_resid_two.astype(BF16))

        def scatter_rows(values):
            return lax.psum_scatter(values, ('z', 'y'), scatter_dimension=1, tiled=True)

        def by_shard(values):
            return values.reshape(n_tp, -1, width)

        d_w_down = dot_tn(inner_act, d_ffn)
        down_piece = scatter_rows(by_shard(d_w_down))
        d_pre, d_b_ffn = geglu_backward(d_ffn, wf_down, act, slope, n_tp)
        d_w_ffn = dot_tn(d_pre, hidden)
        ffn_piece = scatter_rows(by_shard(d_w_ffn))
        d_hidden_sum = sum_halves(d_pre, lambda rows: dot(rows, wt_ffn))
        d_hidden = ALPHA * d_resid_two + d_hidden_sum
        d_ln1_bias = jnp.sum(d_hidden, axis=0)
        d_resid_one, d_ln1_gain = norm_one_pull(d_hidden)
        d_b_out = jnp.sum(d_resid_one, axis=0)
        d_attn = both_halves(d_resid_one.astype(BF16))
        d_context = dot_nt(d_attn, wf_out).astype(BF16)
        d_qkv, d_b_qkv = attention_backward(core, qkv, d_context, cos_tab, sin_tab, blk)

        def column_part(which):
            cols = width // 2
            product = dot(d_qkv, lax.dynamic_slice_in_dim(wt_qkv, which * cols, cols, 1))
            direct = ALPHA * lax.dynamic_slice_in_dim(d_resid_one, which * cols, cols, 1)
            return product + jnp.concatenate([direct, jnp.zeros_like(direct)], axis=0)

        sent = column_part(1 - ci)
        other_rows = jnp.concatenate([swap(sent[half:]), swap(sent[:half])], axis=0)
        d_rows = lax.optimization_barrier(column_part(ci)) + other_rows
        from_left, from_right = lax.ppermute(d_rows, 'x', right), lax.ppermute(d_rows, 'x', left)
        d_rows, d_qkv, d_attn = lax.optimization_barrier((d_rows, d_qkv, d_attn))
        d_w_qkv = dot_tn(d_qkv, emb)
        d_w_out = dot_tn(context, d_attn)

        def small_split(values):
            return jnp.pad(values, ((0, 0), (0, -values.shape[1] % (n_q * 8 * width)))).reshape(n_tp, -1, width)

        vec5 = jnp.concatenate([d_b_out, d_ln1_gain, d_ln1_bias, d_b_down, d_ln2_gain])
        small = jnp.concatenate([
            jnp.broadcast_to(vec5, (n_tp, vec5.shape[0])),
            d_b_ffn.reshape(n_tp, -1), d_b_qkv.reshape(n_tp, -1)], axis=1)

        def to_shard(piece):
            total = lax.dynamic_index_in_dim(piece, xi, 0, keepdims=False)
            for step in range(1, n_tp):
                shift = [(i, (i + step) % n_tp) for i in range(n_tp)]
                total = total + lax.ppermute(lax.dynamic_index_in_dim(piece, (xi + step) % n_tp, 0, keepdims=False), 'x', shift)
            return total

        attn = jnp.concatenate([by_shard(d_w_qkv), by_shard(d_w_out), small_split(small)], axis=1)

        attn = scatter_rows(attn)
        far_top = lax.ppermute(from_left[:half], 'x', right)
        far_low = lax.ppermute(from_right[half:], 'x', left)
        row_lists, row_counts = bucket_ids(target_ids, n_tp, vocab_loc)
        d_table = add_rows(row_lists, row_counts, [d_rows, from_left, from_right, far_top, far_low], vocab_loc)
        down_piece, ffn_piece, attn, d_table = lax.optimization_barrier((down_piece, ffn_piece, attn, d_table))
        d_table = lax.psum(d_table, ('z', 'y'))
        down_piece, gate_lin_piece, attn_piece = [to_shard(piece) for piece in (down_piece, ffn_piece, attn)]

        def gather_rows(values, order):
            sizes = {'z': n_z, 'y': n_y}
            for depth, axis in enumerate(order):
                values = in_order(ring_blocks(values, axis, sizes[axis], split=depth == 1), axis, sizes[axis])
            if order == 'zy':
                values = jnp.swapaxes(values, 0, 1)
            values = values.reshape(n_q, -1, width)
            return in_order([(0, values), (1, swap(values))], 'c', 2)

        mixed = gather_rows(jnp.concatenate([down_piece, attn_piece], axis=0), 'yz')
        n_down = down_piece.shape[0]
        d_w_down = mixed[:, :, :n_down].reshape(-1, width)
        gate_lin = gather_rows(gate_lin_piece, 'zy').reshape(2, -1, width)
        d_w_gate = gate_lin[:, :ffn_cols].reshape(-1, width).T
        d_w_lin = gate_lin[:, ffn_cols:].reshape(-1, width).T
        attn = mixed[:, :, n_down:].reshape(2, -1, width)
        out_rows = w_out.shape[0] // 2
        d_w_qkv = jnp.concatenate([head_order(attn[i, :qkv_cols], pairs_loc) for i in (0, 1)], axis=0).T
        d_w_out = attn[:, qkv_cols:qkv_cols + out_rows].reshape(-1, width)
        small = attn[:, qkv_cols + out_rows:].reshape(2, -1)
        d_b_out, d_ln1_gain, d_ln1_bias, d_b_down, d_ln2_gain = [
            small[0, i * width:(i + 1) * width] + small[1, i * width:(i + 1) * width] for i in range(5)]
        at = 5 * width
        d_b_gate = small[:, at:at + ffn_cols].reshape(-1)
        d_b_lin = small[:, at + ffn_cols:at + 2 * ffn_cols].reshape(-1)
        at += 2 * ffn_cols
        d_b_qkv = jnp.concatenate([head_order(small[i, at:at + qkv_cols], pairs_loc) for i in (0, 1)]).reshape(heads_loc, -1)
        base = jnp.zeros((vocab_loc, width), F32)
        d_table, base, d_w_qkv, d_w_out, d_w_gate, d_w_lin, d_w_down = lax.optimization_barrier((d_table, base, d_w_qkv, d_w_out, d_w_gate, d_w_lin, d_w_down))
        cols = width // 2
        other_table = [swap(part) for part in d_table]
        span = vocab_loc // 4
        for parts, which in ((d_table, ci), (other_table, 1 - ci)):
            for index, part in enumerate(parts):
                base = lax.dynamic_update_slice(base, SHRINK * part, (jnp.int32(index * span), which * cols))
        d_table = base
        return (d_table, d_w_qkv, d_b_qkv, d_w_out, d_b_out, d_ln1_gain, d_ln1_bias, d_w_gate, d_b_gate, d_w_lin, d_b_lin, d_w_down, d_b_down, d_ln2_gain)

    return jax.shard_map(device_step, mesh=fine, in_specs=in_specs, out_specs=out_specs, check_vma=False)
```

```python
import functools

import jax
import jax.numpy as jnp
from jax import lax
from jax.experimental import pallas as pl
from jax.experimental.pallas import tpu as pltpu
from jax.sharding import Mesh, PartitionSpec as P


ALPHA = 140.0 ** 0.5
EPS = 1e-5
SHRINK = 0.1
ROPE_BASE = 10000.0
F32 = jnp.float32
BF16 = jnp.bfloat16
SWAP = ((0, 1), (1, 0))


def swap(values):
    return lax.ppermute(values, 'c', SWAP)


def unit():
    return 1.0 + (lax.axis_index('x') // lax.axis_size('x')).astype(F32)


def rounded(values):
    return (values * unit()).astype(BF16)


def norm_scaled(values, gain):
    mean_val = jnp.mean(values, axis=-1, keepdims=True)
    centered = values - mean_val
    variance = jnp.mean(centered * centered, axis=-1, keepdims=True)
    return centered * lax.rsqrt(variance + EPS) * gain


def dot(left, right):
    return jnp.dot(left, right, preferred_element_type=F32)


def dot_tn(left, right):
    return lax.dot_general(left, right, (((0,), (0,)), ((), ())), preferred_element_type=F32)


def dot_nt(left, right):
    return lax.dot_general(left, right, (((1,), (1,)), ((), ())), preferred_element_type=F32)


def rope_tables(seq_len, head_dim):
    half_dim = head_dim // 2
    inv_freq = ROPE_BASE ** (-2.0 * jnp.arange(half_dim, dtype=F32) / head_dim)
    angles = jnp.arange(seq_len, dtype=F32)[:, None] * inv_freq[None, :]
    cos, sin = jnp.cos(angles), jnp.sin(angles)
    return jnp.concatenate([cos, cos, cos, cos], axis=1), jnp.concatenate([-sin, sin, -sin, sin], axis=1)


def lanes_of_head(rows, head):
    lane = lax.broadcasted_iota(jnp.int32, (rows, 128), 1)
    return (lane >= 64) if head else (lane < 64)


def rotate(values):
    lane = lax.broadcasted_iota(jnp.int32, values.shape, 1)
    return jnp.where(lane % 64 < 32, pltpu.roll(values, 96, axis=1), pltpu.roll(values, 32, axis=1))


def only_head(values, head):
    return jnp.where(lanes_of_head(values.shape[0], head), values, jnp.zeros_like(values))


def stage_qkv(core, half, qkv_ref, cos_ref, sin_ref, q_scr, k_scr, v_scr):
    for part in (0, 1):
        local = pl.ds(part * half, half)
        place = pl.ds(pl.multiple_of((core * half + part * half) % (2 * half), half), half)
        cos, sin = cos_ref[place, :], sin_ref[place, :]
        q = qkv_ref[local, 0:128].astype(F32)
        k = qkv_ref[local, 128:256].astype(F32)
        q_scr[place, :] = (q * cos + rotate(q) * sin).astype(BF16) * BF16(0.125)
        k_scr[place, :] = (k * cos + rotate(k) * sin).astype(BF16)
        v_scr[place, :] = qkv_ref[local, 256:384]


def softmax_rows(q_h, k_scr, row0, rows):
    s_diag = dot_nt(q_h, k_scr[row0:row0 + rows, :])
    keep = lax.broadcasted_iota(jnp.int32, (rows, rows), 0) >= lax.broadcasted_iota(jnp.int32, (rows, rows), 1)
    scores = jnp.where(keep, s_diag, -1e30)
    if row0:
        scores = jnp.concatenate([dot_nt(q_h, k_scr[0:row0, :]), scores], axis=1)
    top = jnp.max(scores, axis=1, keepdims=True)
    weights = jnp.exp(scores - top)
    total = jnp.sum(weights, axis=1, keepdims=True)
    return (weights * (1.0 / total)).astype(BF16)


def attn_fwd_kernel(half, rows, core_ref, qkv_ref, cos_ref, sin_ref, ctx_ref, q_scr, k_scr, v_scr, ctx_scr):
    core = core_ref[0]
    seq_len = 2 * half
    stage_qkv(core, half, qkv_ref, cos_ref, sin_ref, q_scr, k_scr, v_scr)
    for row0 in range(0, seq_len, rows):
        q_blk = q_scr[row0:row0 + rows, :]
        v_blk = v_scr[0:row0 + rows, :]
        ctx = jnp.zeros((rows, 128), F32)
        for head in (0, 1):
            probs = softmax_rows(only_head(q_blk, head), k_scr, row0, rows)
            ctx = jnp.where(lanes_of_head(rows, head), dot(probs, v_blk), ctx)
        ctx_scr[row0:row0 + rows, :] = ctx.astype(BF16)
    for part in (0, 1):
        place = pl.ds(pl.multiple_of((core * half + part * half) % seq_len, half), half)
        ctx_ref[part * half:(part + 1) * half, :] = ctx_scr[place, :]


def attn_bwd_kernel(half, rows, core_ref, qkv_ref, dctx_ref, cos_ref, sin_ref, dqkv_ref, dbias_ref,
                    q_scr, k_scr, v_scr, do_scr, dq_scr, dk_scr, dv_scr):
    core = core_ref[0]
    seq_len = 2 * half
    stage_qkv(core, half, qkv_ref, cos_ref, sin_ref, q_scr, k_scr, v_scr)
    for part in (0, 1):
        place = pl.ds(pl.multiple_of((core * half + part * half) % seq_len, half), half)
        do_scr[place, :] = dctx_ref[part * half:(part + 1) * half, :]
    dk_scr[...] = jnp.zeros_like(dk_scr)
    dv_scr[...] = jnp.zeros_like(dv_scr)
    for row0 in range(0, seq_len, rows):
        end = row0 + rows
        q_blk = q_scr[row0:end, :]
        do_blk = do_scr[row0:end, :]
        k_blk = k_scr[0:end, :]
        v_blk = v_scr[0:end, :]
        dq = jnp.zeros((rows, 128), F32)
        for head in (0, 1):
            q_h = only_head(q_blk, head)
            do_h = only_head(do_blk, head)
            probs = softmax_rows(q_h, k_scr, row0, rows)
            d_probs = dot_nt(do_h, v_blk)
            probs_f = probs.astype(F32)
            inner = jnp.sum(d_probs * probs_f, axis=1, keepdims=True)
            d_scores = (probs_f * (d_probs - inner)).astype(BF16)
            dq = jnp.where(lanes_of_head(rows, head), dot(d_scores, k_blk), dq)
            dk_scr[0:end, :] += dot_tn(d_scores, q_h)
            dv_scr[0:end, :] += dot_tn(probs, do_h)
        dq_scr[row0:end, :] = dq * 0.125
    for part in (0, 1):
        place = pl.ds(pl.multiple_of((core * half + part * half) % seq_len, half), half)
        cos, sin = cos_ref[place, :], -sin_ref[place, :]
        dq, dk, dv = dq_scr[place, :], dk_scr[place, :], dv_scr[place, :]
        dq = dq * cos + rotate(dq) * sin
        dk = dk * cos + rotate(dk) * sin
        for place_out, grad in ((0, dq), (128, dk), (256, dv)):
            dqkv_ref[part * half:(part + 1) * half, place_out:place_out + 128] = grad.astype(BF16)
            total = jnp.sum(grad, axis=0, keepdims=True)
            if part:
                dbias_ref[0:1, place_out:place_out + 128] += total
            else:
                dbias_ref[0:1, place_out:place_out + 128] = total


def attention_forward(core, qkv, cos_tab, sin_tab, rows):
    seq_len, width = qkv.shape
    pairs = width // 384
    full = pl.BlockSpec((seq_len, 128), lambda p, c: (0, 0))
    return pl.pallas_call(
        functools.partial(attn_fwd_kernel, seq_len // 2, rows),
        grid_spec=pltpu.PrefetchScalarGridSpec(
            num_scalar_prefetch=1,
            grid=(pairs,),
            in_specs=[pl.BlockSpec((seq_len, 384), lambda p, c: (0, p)), full, full],
            out_specs=pl.BlockSpec((seq_len, 128), lambda p, c: (0, p)),
            scratch_shapes=[pltpu.VMEM((seq_len, 128), BF16)] * 4,
        ),
        out_shape=jax.ShapeDtypeStruct((seq_len, pairs * 128), BF16),
        compiler_params=pltpu.CompilerParams(vmem_limit_bytes=48 * 1024 * 1024),
        cost_estimate=pl.CostEstimate(flops=seq_len * seq_len * 128 * 4 * pairs, bytes_accessed=seq_len * width * 3, transcendentals=seq_len * seq_len * pairs),
        name='attn_fwd',
    )(core, qkv, cos_tab, sin_tab)


def attention_backward(core, qkv, d_ctx, cos_tab, sin_tab, rows):
    seq_len, width = qkv.shape
    pairs = width // 384
    full = pl.BlockSpec((seq_len, 128), lambda p, c: (0, 0))
    return pl.pallas_call(
        functools.partial(attn_bwd_kernel, seq_len // 2, rows),
        grid_spec=pltpu.PrefetchScalarGridSpec(
            num_scalar_prefetch=1,
            grid=(pairs,),
            in_specs=[pl.BlockSpec((seq_len, 384), lambda p, c: (0, p)), pl.BlockSpec((seq_len, 128), lambda p, c: (0, p)), full, full],
            out_specs=[pl.BlockSpec((seq_len, 384), lambda p, c: (0, p)), pl.BlockSpec((1, 384), lambda p, c: (0, p))],
            scratch_shapes=[pltpu.VMEM((seq_len, 128), BF16)] * 4 + [pltpu.VMEM((seq_len, 128), F32)] * 3,
        ),
        out_shape=[jax.ShapeDtypeStruct((seq_len, width), BF16), jax.ShapeDtypeStruct((1, width), F32)],
        compiler_params=pltpu.CompilerParams(vmem_limit_bytes=56 * 1024 * 1024),
        cost_estimate=pl.CostEstimate(flops=seq_len * seq_len * 128 * 10 * pairs, bytes_accessed=seq_len * width * 5, transcendentals=seq_len * seq_len * pairs),
        name='attn_bwd',
    )(core, qkv, d_ctx, cos_tab, sin_tab)


def geglu_fwd_kernel(chunk, hidden_ref, wide_ref, bias_ref, inner_ref, act_ref, slope_ref, weight_ref):
    rows, cols = inner_ref.shape
    weight_ref[...] = wide_ref[...].reshape(weight_ref.shape).astype(BF16)
    for row0 in range(0, rows, chunk):
        place = slice(row0, row0 + chunk)
        part = hidden_ref[place, :]
        gate = dot_nt(part, weight_ref[0:cols, :]) + bias_ref[:, 0:cols]
        lin = dot_nt(part, weight_ref[cols:2 * cols, :]) + bias_ref[:, cols:2 * cols]
        below = 0.5 + 0.5 * lax.erf(gate * (0.5 ** 0.5))
        act = gate * below
        act_ref[place, :] = act
        slope_ref[place, :] = (below + gate * jnp.exp(gate * gate * -0.5) * ((2.0 * jnp.pi) ** -0.5)) * lin
        inner_ref[place, :] = (act * lin).astype(BF16)


def geglu_forward(hidden, weight, bias, groups):
    seq_len, width = hidden.shape
    slices, _, slice_rows, _ = weight.shape
    cols = slices * slice_rows // 2
    tile = pl.BlockSpec((seq_len, cols), lambda i: (0, i))
    shape = (seq_len, groups * cols)
    return pl.pallas_call(
        functools.partial(geglu_fwd_kernel, min(256, seq_len)),
        grid=(groups,),
        in_specs=[pl.BlockSpec((seq_len, width), lambda i: (0, 0)), pl.BlockSpec((slices, 1, slice_rows, width), lambda i: (0, i, 0, 0)), pl.BlockSpec((1, 2 * cols), lambda i: (0, i))],
        out_specs=[tile, tile, tile, pl.BlockSpec((2 * cols, width), lambda i: (i, 0))],
        out_shape=[jax.ShapeDtypeStruct(shape, BF16), jax.ShapeDtypeStruct(shape, F32), jax.ShapeDtypeStruct(shape, F32), jax.ShapeDtypeStruct((2 * shape[1], width), BF16)],
        compiler_params=pltpu.CompilerParams(vmem_limit_bytes=56 * 1024 * 1024),
        cost_estimate=pl.CostEstimate(flops=4 * seq_len * width * shape[1], bytes_accessed=seq_len * shape[1] * 10, transcendentals=2 * seq_len * shape[1]),
        name='geglu_fwd',
    )(hidden, weight, bias)


def geglu_bwd_kernel(chunk, d_ffn_ref, weight_ref, act_ref, slope_ref, grad_ref, sum_ref):
    rows, cols = act_ref.shape
    for row0 in range(0, rows, chunk):
        place = slice(row0, row0 + chunk)
        d_inner = dot_nt(d_ffn_ref[place, :], weight_ref[...]).astype(BF16).astype(F32)
        for at, factor in ((0, slope_ref), (cols, act_ref)):
            grad = d_inner * factor[place, :]
            grad_ref[place, at:at + cols] = grad.astype(BF16)
            total = jnp.sum(grad, axis=0, keepdims=True)
            if row0:
                sum_ref[:, at:at + cols] += total
            else:
                sum_ref[:, at:at + cols] = total


def geglu_backward(d_ffn, weight, act, slope, groups):
    seq_len, width = d_ffn.shape
    cols = weight.shape[0] // groups
    tile = pl.BlockSpec((seq_len, cols), lambda i: (0, i))
    return pl.pallas_call(
        functools.partial(geglu_bwd_kernel, min(256, seq_len)),
        grid=(groups,),
        in_specs=[pl.BlockSpec((seq_len, width), lambda i: (0, 0)), pl.BlockSpec((cols, width), lambda i: (i, 0)), tile, tile],
        out_specs=[pl.BlockSpec((seq_len, 2 * cols), lambda i: (0, i)), pl.BlockSpec((1, 2 * cols), lambda i: (0, i))],
        out_shape=[jax.ShapeDtypeStruct((seq_len, 2 * groups * cols), BF16), jax.ShapeDtypeStruct((1, 2 * groups * cols), F32)],
        compiler_params=pltpu.CompilerParams(vmem_limit_bytes=56 * 1024 * 1024),
        cost_estimate=pl.CostEstimate(flops=2 * seq_len * width * groups * cols, bytes_accessed=seq_len * groups * cols * 12, transcendentals=0),
        name='geglu_bwd',
    )(d_ffn, weight, act, slope)


def bucket_kernel(streams, group_ref, value_ref, list_ref, count_ref):
    size = group_ref.shape[0] // streams
    for slot in range(streams * 5):
        count_ref[slot] = 0

    def place(step, carry):
        spots = []
        for stream in range(streams):
            group = group_ref[stream * size + step]
            spots.append((stream * 5 + group, value_ref[stream * size + step]))
        filled = [count_ref[slot] for slot, _ in spots]
        for (slot, value), at in zip(spots, filled):
            list_ref[slot * size + at] = value
            count_ref[slot] = at + 1
        return carry

    lax.fori_loop(0, size, place, 0)


def index_bits(total):
    return (total - 1).bit_length()


def bucket_ids(ids, streams, vocab):
    total = ids.shape[0]
    size = total // streams
    span = vocab // 4
    group = jnp.where(ids < 0, 4, ids // span)
    value = jnp.where(ids < 0, 0, (ids % span) * (1 << index_bits(total)) + jnp.arange(total, dtype=jnp.int32))
    smem = pl.BlockSpec(memory_space=pltpu.SMEM)
    return pl.pallas_call(
        functools.partial(bucket_kernel, streams),
        in_specs=[smem, smem],
        out_specs=[smem, smem],
        out_shape=[jax.ShapeDtypeStruct((streams * 5 * size,), jnp.int32), jax.ShapeDtypeStruct((streams * 5,), jnp.int32)],
        cost_estimate=pl.CostEstimate(flops=40_000_000, bytes_accessed=20 * total, transcendentals=0),
        name='bucket_ids',
    )(group, value)


def table_kernel(total, streams, list_ref, count_ref, *refs):
    blocks, outs, (rows, bufs, in_sem, out_sem) = refs[:-8], refs[-8:-4], refs[-4:]
    span, width = bufs.shape[1:]
    bits = index_bits(total)
    loads = []
    first = 0
    for index, block in enumerate(blocks):
        loads.append(pltpu.make_async_copy(block, rows.at[pl.ds(first, block.shape[0]), :], in_sem.at[index]))
        first += block.shape[0]
    for load in loads:
        load.start()

    def store(group):
        return pltpu.make_async_copy(bufs.at[group % 2], outs[group], out_sem.at[group % 2])

    for group in range(4):
        buf = bufs.at[group % 2]
        if group >= 2:
            store(group - 2).wait()

        def clear(step, carry):
            buf[pl.ds(pl.multiple_of(step * 8, 8), 8), :] = jnp.zeros((8, width), F32)
            return carry

        lax.fori_loop(0, span // 8, clear, 0, unroll=3 if (span // 8) % 3 == 0 else 1)
        if group == 0:
            for load in loads:
                load.wait()

        for stream in range(streams):
            slot = stream * 5 + group
            first_entry = slot * (total // streams)

            def add_row(index):
                packed = list_ref[first_entry + index]
                target = lax.shift_right_logical(packed, bits)
                source = packed & ((1 << bits) - 1)
                buf[pl.ds(target, 1), :] += rows[pl.ds(source, 1), :]

            def add_four(step, carry):
                for k in range(4):
                    add_row(step * 4 + k)
                return carry

            def add_one(index, carry):
                add_row(index)
                return carry

            count = count_ref[slot]
            quads = lax.shift_right_logical(count, 2)
            lax.fori_loop(0, quads, add_four, 0)
            lax.fori_loop(quads * 4, count, add_one, 0)
        store(group).start()
    store(2).wait()
    store(3).wait()


def add_rows(lists, counts, blocks, vocab):
    width = blocks[0].shape[1]
    total = sum(block.shape[0] for block in blocks)
    span = vocab // 4
    return pl.pallas_call(
        functools.partial(table_kernel, total, counts.shape[0] // 5),
        grid_spec=pltpu.PrefetchScalarGridSpec(
            num_scalar_prefetch=2,
            grid=(),
            in_specs=[pl.BlockSpec(memory_space=pl.ANY)] * len(blocks),
            out_specs=[pl.BlockSpec(memory_space=pl.ANY)] * 4,
            scratch_shapes=[pltpu.VMEM((total, width), F32), pltpu.VMEM((2, span, width), F32), pltpu.SemaphoreType.DMA((len(blocks),)), pltpu.SemaphoreType.DMA((2,))],
        ),
        out_shape=[jax.ShapeDtypeStruct((span, width), F32)] * 4,
        compiler_params=pltpu.CompilerParams(vmem_limit_bytes=44 * 1024 * 1024),
        cost_estimate=pl.CostEstimate(flops=30 * vocab * width, bytes_accessed=4 * vocab * width, transcendentals=0),
        name='table_rows',
    )(lists, counts, *blocks)


def ring_blocks(values, axis, n, split=True):
    if n == 1:
        return [(0, values)]
    right = [(i, (i + 1) % n) for i in range(n)]
    left = [(i, (i - 1) % n) for i in range(n)]
    if n == 2:
        return [(0, values), (1, lax.ppermute(values, axis, right))]
    from_left, from_right = lax.ppermute(values, axis, right), lax.ppermute(values, axis, left)
    mid = values.shape[0] // 2
    if split:
        far = jnp.concatenate([lax.ppermute(from_left[:mid], axis, right), lax.ppermute(from_right[mid:], axis, left)], axis=0)
    else:
        far = lax.ppermute(values, axis, [(i, (i + 2) % n) for i in range(n)])
    return [(0, values), (-1, from_left), (1, from_right), (2, far)]


def in_order(blocks, axis, n):
    if n == 1:
        return blocks[0][1][None]
    whole = jnp.zeros((n,) + blocks[0][1].shape, blocks[0][1].dtype)
    for offset, block in blocks:
        whole = lax.dynamic_update_index_in_dim(whole, block, (lax.axis_index(axis) + offset) % n, 0)
    return whole


def pair_order(rows, n_pairs):
    split = rows.reshape(n_pairs, 2, 3, 64, *rows.shape[1:])
    return jnp.swapaxes(split, 1, 2).reshape(rows.shape)


def head_order(rows, n_pairs):
    split = rows.reshape(n_pairs, 3, 2, 64, *rows.shape[1:])
    return jnp.swapaxes(split, 1, 2).reshape(rows.shape)


def solution(mesh):
    n_tp = mesh.shape['tp']
    n_dp = mesh.shape['dp']
    n_q = n_dp // 2
    n_z = 4 if n_q >= 16 else n_q
    n_y = n_q // n_z
    fine = Mesh(mesh.devices.reshape(n_tp, n_z, n_y, 2), ('x', 'z', 'y', 'c'))
    col, row, rep, vec = P(None, 'x'), P('x', None), P(), P('x')
    weight_specs = (col, row, row, rep, rep, rep, col, vec, col, vec, row, rep, rep)
    in_specs = (P(('z', 'y', 'c'), None), P(('z', 'y', 'c'), None, None), row) + weight_specs
    out_specs = (row,) + weight_specs

    def device_step(tokens, cotangent, emb_table, w_qkv, b_qkv, w_out, b_out, ln1_gain, ln1_bias, w_gate, b_gate, w_lin, b_lin, w_down, b_down, ln2_gain):
        xi, ci = lax.axis_index('x'), lax.axis_index('c')
        qi = lax.axis_index(('z', 'y'))
        seqs, seq_len = tokens.shape
        half = seq_len // 2
        vocab_loc, width = emb_table.shape
        heads_loc = b_qkv.shape[0]
        pairs_loc = heads_loc // 4

        def half_of(values, which, axis):
            size = values.shape[axis] // 2
            return lax.dynamic_slice_in_dim(values, which * size, size, axis)

        def share(values, axis):
            size = values.shape[axis] // n_q
            return lax.dynamic_slice_in_dim(values, qi * size, size, axis)

        qkv_cols = w_qkv.shape[1] // 2
        ffn_cols = w_gate.shape[1] // 2
        bias_rows = jnp.concatenate([
            pair_order(half_of(b_qkv.astype(F32), ci, 0).reshape(-1), pairs_loc),
            half_of(b_gate.astype(F32), ci, 0), half_of(b_lin.astype(F32), ci, 0)])
        bias_rows = jnp.pad(bias_rows, (0, -bias_rows.shape[0] % (8 * width))).reshape(-1, width)
        gate_lin = jnp.concatenate([half_of(w_gate, ci, 1), half_of(w_lin, ci, 1)], axis=1)
        parts = [
            share(pair_order(half_of(w_qkv, ci, 1).T, pairs_loc), 0),
            share(half_of(w_out, ci, 0), 0),
            share(gate_lin, 1).T]
        starts = [bias_rows.shape[0]]
        for part in parts:
            starts.append(starts[-1] + part.shape[0])
        packed = jnp.concatenate([bias_rows] + [part.astype(F32) for part in parts], axis=0)
        packed_blocks = ring_blocks(packed, 'x', n_tp, split=False)

        other_tokens = swap(tokens)
        line_tokens = jnp.where(ci == 0, jnp.concatenate([tokens, other_tokens], axis=0), jnp.concatenate([other_tokens, tokens], axis=0)) - xi * vocab_loc
        line_ids = half_of(line_tokens, ci, 1)
        in_shard = (line_ids >= 0) & (line_ids < vocab_loc)
        safe_ids = jnp.where(in_shard, line_ids, 0)
        right = [(i, (i + 1) % n_tp) for i in range(n_tp)]
        left = [(i, (i - 1) % n_tp) for i in range(n_tp)]
        quarter = half // 2
        steps = jnp.arange(1, n_tp + 1, dtype=jnp.int32)
        ring_ids = jnp.stack([
            jnp.take(safe_ids[:, :quarter], (xi - steps) % n_tp, axis=0),
            jnp.take(safe_ids[:, quarter:], (xi + steps) % n_tp, axis=0)], axis=1)
        ring_here = jnp.stack([
            jnp.take(in_shard[:, :quarter], (xi - steps) % n_tp, axis=0),
            jnp.take(in_shard[:, quarter:], (xi + steps) % n_tp, axis=0)], axis=1)
        first_ids, later_ids = ring_ids[:1].reshape(-1), ring_ids[1:].reshape(-1)
        first = emb_table.at[first_ids].get(mode='promise_in_bounds')
        offsets = [offset for offset, _ in packed_blocks]
        first, later_ids, packed_values = lax.optimization_barrier((first, later_ids, [block for _, block in packed_blocks]))
        packed = in_order(list(zip(offsets, packed_values)), 'x', n_tp)

        def gather_q(values):
            whole = lax.all_gather(values.reshape(-1, width), ('z', 'y'), axis=0, tiled=True)
            return whole.reshape(n_q, n_tp, -1, width)

        def weight(gathered, lo, hi):
            return rounded(jnp.swapaxes(gathered[:, :, lo:hi], 0, 1).reshape(-1, width))

        attn_all, ffn_all = gather_q(packed[:, :starts[2]]), gather_q(packed[:, starts[2]:])
        wt_qkv = weight(attn_all, starts[0], starts[1])
        wf_out = weight(attn_all, starts[1], starts[2])
        bias_all = attn_all[0, :, :starts[0]].reshape(n_tp, -1)
        bf_qkv = bias_all[:, :qkv_cols].reshape(1, -1)
        bf_ffn = bias_all[:, qkv_cols:qkv_cols + 2 * ffn_cols].reshape(1, -1)

        later = emb_table.at[later_ids].get(mode='promise_in_bounds').reshape(n_tp - 1, 2, quarter, width)
        first = first.reshape(2, quarter, width)

        def masked(found, step, way):
            return jnp.where(ring_here[step, way][:, None], found.astype(F32), 0.0)

        top_sum, low_sum = masked(first[0], 0, 0), masked(first[1], 0, 1)
        cos_tab, sin_tab = rope_tables(seq_len, 64)
        order = (xi + jnp.array([0, n_tp - 1, 1, 2], jnp.int32)) % n_tp
        target_ids = jnp.concatenate([line_ids, half_of(line_tokens, 1 - ci, 1)], axis=1)
        target_ids = jnp.where((target_ids >= 0) & (target_ids < vocab_loc), target_ids, -1)
        target_ids = jnp.take(target_ids, order, axis=0).reshape(-1)
        for step in range(1, n_tp):
            top_in, low_in = lax.ppermute(top_sum, 'x', right), lax.ppermute(low_sum, 'x', left)
            if step == 3:
                top_in, low_in, wt_qkv, wf_out, bf_qkv, bf_ffn, cos_tab, sin_tab = lax.optimization_barrier(
                    (top_in, low_in, wt_qkv, wf_out, bf_qkv, bf_ffn, cos_tab, sin_tab))
            top_sum = top_in + masked(later[step - 1, 0], step, 0)
            low_sum = low_in + masked(later[step - 1, 1], step, 1)
        e_own = jnp.concatenate([top_sum, low_sum], axis=0)

        down_own = half_of(w_down, ci, 0).astype(F32)
        e_own, down_own = lax.optimization_barrier((e_own, down_own))
        down_left, down_right = lax.ppermute(down_own, 'x', right), lax.ppermute(down_own, 'x', left)

        g_seq = lax.dynamic_slice_in_dim(cotangent, xi % seqs, 1, 0)[0]
        g_other = swap(half_of(g_seq, 1 - ci, 0).astype(F32))
        g_own = jnp.where(xi // seqs == ci, half_of(g_seq, ci, 0).astype(F32), g_other)

        core = ci.astype(jnp.int32).reshape(1)
        blk = min(256, half)

        def both_halves(own):
            wide = own.astype(F32)
            return jnp.concatenate([own, rounded(swap(wide))], axis=0)

        def sum_halves(left, right_of):
            other = swap(right_of(left[half:]))
            return lax.optimization_barrier(right_of(left[:half])) + other

        emb = both_halves(e_own.astype(BF16))
        qkv = (dot_nt(emb, wt_qkv) + bf_qkv).astype(BF16)
        context = attention_forward(core, qkv, cos_tab, sin_tab, blk)
        context, down_left, down_right = lax.optimization_barrier((context, down_left, down_right))
        mid = ffn_cols // 2
        down_top, down_low = lax.ppermute(down_left[:mid], 'x', right), lax.ppermute(down_right[mid:], 'x', left)
        near = in_order([(0, rounded(down_own)), (-1, rounded(down_left)), (1, rounded(down_right))], 'x', n_tp)
        attn_out = sum_halves(context, lambda rows: dot(rows, wf_out)) + b_out.astype(F32)
        normed_one, norm_one_pull = jax.vjp(norm_scaled, ALPHA * e_own + attn_out, ln1_gain.astype(F32))
        z_own = (normed_one + ln1_bias.astype(F32)).astype(BF16)
        hidden = both_halves(z_own)
        inner_act, act, slope, wt_ffn = geglu_forward(hidden, ffn_all, bf_ffn, n_tp)
        inner_act, down_top, down_low = lax.optimization_barrier((inner_act, down_top, down_low))
        wf_down = lax.dynamic_update_index_in_dim(near, rounded(jnp.concatenate([down_top, down_low], axis=0)), (xi + 2) % n_tp, 0).reshape(-1, width)
        ffn_out = sum_halves(inner_act, lambda rows: dot(rows, wf_down)) + b_down.astype(F32)
        norm_two_pull = jax.vjp(norm_scaled, ALPHA * z_own.astype(F32) + ffn_out, ln2_gain.astype(F32))[1]

        d_resid_two, d_ln2_gain = norm_two_pull(g_own)
        d_b_down = jnp.sum(d_resid_two, axis=0)
        d_ffn = both_halves(d_resid_two.astype(BF16))

        def scatter_rows(values):
            return lax.psum_scatter(values, ('z', 'y'), scatter_dimension=1, tiled=True)

        def by_shard(values):
            return values.reshape(n_tp, -1, width)

        d_w_down = dot_tn(inner_act, d_ffn)
        down_piece = scatter_rows(by_shard(d_w_down))
        d_pre, d_b_ffn = geglu_backward(d_ffn, wf_down, act, slope, n_tp)
        d_w_ffn = dot_tn(d_pre, hidden)
        ffn_piece = scatter_rows(by_shard(d_w_ffn))
        d_hidden_sum = sum_halves(d_pre, lambda rows: dot(rows, wt_ffn))
        d_hidden = ALPHA * d_resid_two + d_hidden_sum
        d_ln1_bias = jnp.sum(d_hidden, axis=0)
        d_resid_one, d_ln1_gain = norm_one_pull(d_hidden)
        d_b_out = jnp.sum(d_resid_one, axis=0)
        d_attn = both_halves(d_resid_one.astype(BF16))
        d_context = dot_nt(d_attn, wf_out).astype(BF16)
        d_qkv, d_b_qkv = attention_backward(core, qkv, d_context, cos_tab, sin_tab, blk)

        def column_part(which):
            cols = width // 2
            product = dot(d_qkv, lax.dynamic_slice_in_dim(wt_qkv, which * cols, cols, 1))
            direct = ALPHA * lax.dynamic_slice_in_dim(d_resid_one, which * cols, cols, 1)
            return product + jnp.concatenate([direct, jnp.zeros_like(direct)], axis=0)

        sent = column_part(1 - ci)
        other_rows = jnp.concatenate([swap(sent[half:]), swap(sent[:half])], axis=0)
        d_rows = lax.optimization_barrier(column_part(ci)) + other_rows
        from_left, from_right = lax.ppermute(d_rows, 'x', right), lax.ppermute(d_rows, 'x', left)
        d_rows, d_qkv, d_attn = lax.optimization_barrier((d_rows, d_qkv, d_attn))
        d_w_qkv = dot_tn(d_qkv, emb)
        d_w_out = dot_tn(context, d_attn)

        def small_split(values):
            return jnp.pad(values, ((0, 0), (0, -values.shape[1] % (n_q * 8 * width)))).reshape(n_tp, -1, width)

        vec5 = jnp.concatenate([d_b_out, d_ln1_gain, d_ln1_bias, d_b_down, d_ln2_gain])
        small = jnp.concatenate([
            jnp.broadcast_to(vec5, (n_tp, vec5.shape[0])),
            d_b_ffn.reshape(n_tp, -1), d_b_qkv.reshape(n_tp, -1)], axis=1)

        def to_shard(piece):
            total = lax.dynamic_index_in_dim(piece, xi, 0, keepdims=False)
            for step in range(1, n_tp):
                shift = [(i, (i + step) % n_tp) for i in range(n_tp)]
                total = total + lax.ppermute(lax.dynamic_index_in_dim(piece, (xi + step) % n_tp, 0, keepdims=False), 'x', shift)
            return total

        attn = jnp.concatenate([by_shard(d_w_qkv), by_shard(d_w_out), small_split(small)], axis=1)

        attn = scatter_rows(attn)
        far_top = lax.ppermute(from_left[:half], 'x', right)
        far_low = lax.ppermute(from_right[half:], 'x', left)
        row_lists, row_counts = bucket_ids(target_ids, n_tp, vocab_loc)
        d_table = add_rows(row_lists, row_counts, [d_rows, from_left, from_right, far_top, far_low], vocab_loc)
        down_piece, ffn_piece, attn, d_table = lax.optimization_barrier((down_piece, ffn_piece, attn, d_table))
        d_table = lax.psum(d_table, ('z', 'y'))
        down_piece, gate_lin_piece, attn_piece = [to_shard(piece) for piece in (down_piece, ffn_piece, attn)]

        def gather_rows(values, order):
            sizes = {'z': n_z, 'y': n_y}
            for depth, axis in enumerate(order):
                values = in_order(ring_blocks(values, axis, sizes[axis], split=depth == 1), axis, sizes[axis])
            if order == 'zy':
                values = jnp.swapaxes(values, 0, 1)
            values = values.reshape(n_q, -1, width)
            return in_order([(0, values), (1, swap(values))], 'c', 2)

        mixed = gather_rows(jnp.concatenate([down_piece, attn_piece], axis=0), 'yz')
        n_down = down_piece.shape[0]
        d_w_down = mixed[:, :, :n_down].reshape(-1, width)
        gate_lin = gather_rows(gate_lin_piece, 'zy').reshape(2, -1, width)
        d_w_gate = gate_lin[:, :ffn_cols].reshape(-1, width).T
        d_w_lin = gate_lin[:, ffn_cols:].reshape(-1, width).T
        attn = mixed[:, :, n_down:].reshape(2, -1, width)
        out_rows = w_out.shape[0] // 2
        d_w_qkv = jnp.concatenate([head_order(attn[i, :qkv_cols], pairs_loc) for i in (0, 1)], axis=0).T
        d_w_out = attn[:, qkv_cols:qkv_cols + out_rows].reshape(-1, width)
        small = attn[:, qkv_cols + out_rows:].reshape(2, -1)
        d_b_out, d_ln1_gain, d_ln1_bias, d_b_down, d_ln2_gain = [
            small[0, i * width:(i + 1) * width] + small[1, i * width:(i + 1) * width] for i in range(5)]
        at = 5 * width
        d_b_gate = small[:, at:at + ffn_cols].reshape(-1)
        d_b_lin = small[:, at + ffn_cols:at + 2 * ffn_cols].reshape(-1)
        at += 2 * ffn_cols
        d_b_qkv = jnp.concatenate([head_order(small[i, at:at + qkv_cols], pairs_loc) for i in (0, 1)]).reshape(heads_loc, -1)
        base = jnp.zeros((vocab_loc, width), F32)
        d_table, d_w_gate, d_w_lin, d_w_down = lax.optimization_barrier((d_table, d_w_gate, d_w_lin, d_w_down))
        cols = width // 2
        other_table = [swap(part) for part in d_table]
        span = vocab_loc // 4
        for parts, which in ((d_table, ci), (other_table, 1 - ci)):
            for index, part in enumerate(parts):
                base = lax.dynamic_update_slice(base, SHRINK * part, (jnp.int32(index * span), which * cols))
        d_table = base
        return (d_table, d_w_qkv, d_b_qkv, d_w_out, d_b_out, d_ln1_gain, d_ln1_bias, d_w_gate, d_b_gate, d_w_lin, d_b_lin, d_w_down, d_b_down, d_ln2_gain)

    return jax.shard_map(device_step, mesh=fine, in_specs=in_specs, out_specs=out_specs, check_vma=False)
```
